32 devices in a mesh: rep: 2 (over z, core), dp: 16 (over x, y).
Axes of the slice: x: 4, y: 4, z: 1, core: 2. Of those that a mesh axis runs over, the one named last changes fastest.
The devices are a block of a 4x4x8 slice.
Arguments:
- x: bfloat16 [32, 2048, 1024], P(('rep', 'dp')), parts along dimension 0
- dy: bfloat16 [32, 2048, 1024], P(('rep', 'dp')), parts along dimension 0
- w_gate: bfloat16 [2, 1024, 3200], replicated
- w_up: bfloat16 [2, 1024, 3200], replicated
- w_down: bfloat16 [2, 3200, 1024], replicated
- m_w_gate: float32 [2, 1024, 3200], P(None, 'dp')
- m_w_up: float32 [2, 1024, 3200], P(None, 'dp')
- m_w_down: float32 [2, 3200, 1024], P(None, 'dp')
- v_w_gate: float32 [2, 1024, 3200], P(None, 'dp')
- v_w_up: float32 [2, 1024, 3200], P(None, 'dp')
- v_w_down: float32 [2, 3200, 1024], P(None, 'dp')
Outputs:
- output 1: bfloat16 [4, 1024, 3200], P('rep'), parts along dimension 0
- output 2: bfloat16 [4, 1024, 3200], P('rep'), parts along dimension 0
- output 3: bfloat16 [4, 3200, 1024], P('rep'), parts along dimension 0
- output 4: float32 [4, 1024, 3200], P('rep', 'dp'), parts along dimension 0
- output 5: float32 [4, 1024, 3200], P('rep', 'dp'), parts along dimension 0
- output 6: float32 [4, 3200, 1024], P('rep', 'dp'), parts along dimension 0
- output 7: float32 [4, 1024, 3200], P('rep', 'dp'), parts along dimension 0
- output 8: float32 [4, 1024, 3200], P('rep', 'dp'), parts along dimension 0
- output 9: float32 [4, 3200, 1024], P('rep', 'dp'), parts along dimension 0
There are 2 independent parts. The reference program is written for one: setup_inputs(seed, part) draws one part's arguments, and reference() takes and returns one part's arrays. A program takes and returns all parts, laid end to end along the dimension named above; an argument that names none is the same for every part.
All inputs are finite; a program needn't handle non-finite values.
Results may differ from the reference program's by a relative error of at most 0.022.
Values are sent between devices in bfloat16 or wider.
A program may use at most 768 MiB of HBM per device.

```python
import jax
import jax.numpy as jnp
from jax import lax

SEQUENCES = 16
TOKENS = 2048
D = 1024
FF = 3200
LAYERS = 2
NAMES = ("w_gate", "w_up", "w_down")
SHAPES = {"w_gate": (LAYERS, D, FF), "w_up": (LAYERS, D, FF), "w_down": (LAYERS, FF, D)}


def bump(key, n, height):
    away = (jnp.arange(n, dtype=jnp.int32) - jax.random.randint(key, (), 0, n, jnp.int32)) % n
    return jnp.where(away < n // 8, height, 1.0)


def together(key, own, strength):
    shared = jax.random.normal(key, own.shape[1:], jnp.float32)
    return (own + strength * shared) * lax.rsqrt(1 + strength * strength)


def setup_inputs(seed: int = 0, part: int = 0) -> dict:
    kx, kdy, ka, kb, kz, kf, kh, kl, *keys = jax.random.split(jax.random.key(seed), 8 + 3 * len(NAMES))
    kx, kdy, ka, kb = (jax.random.fold_in(k, part) for k in (kx, kdy, ka, kb))
    kw, km, kv = (keys[i::3] for i in range(3))
    shape = (SEQUENCES, TOKENS, D)
    much_x, much_dy = jax.random.uniform(kz, (2,), jnp.float32, 0.0, 1.0)
    loud = 2.0 ** jax.random.uniform(jax.random.fold_in(kz, 1), (), jnp.float32, -1.0, 2.0)
    layers = 2.0 ** jax.random.uniform(kl, (LAYERS, 1, 1), jnp.float32, -1.0, 1.0)
    x = together(ka, jax.random.normal(kx, shape, jnp.float32), much_x) * bump(kf, D, 4.0)
    dy = together(kb, jax.random.normal(kdy, shape, jnp.float32), much_dy)
    drawn = {"x": x.astype(jnp.bfloat16), "dy": (loud * dy * (SEQUENCES * TOKENS) ** -0.5).astype(jnp.bfloat16)}
    for key, name in zip(kw, NAMES, strict=True):
        w = jax.random.normal(key, SHAPES[name], jnp.float32) * SHAPES[name][1] ** -0.5
        drawn[name] = (w * {"w_gate": 1.0, "w_up": bump(kh, FF, 4.0), "w_down": layers}[name]).astype(jnp.bfloat16)
    for key, name in zip(km, NAMES, strict=True):
        drawn[f"m_{name}"] = 0.1 * jax.random.normal(key, SHAPES[name], jnp.float32)
    for key, name in zip(kv, NAMES, strict=True):
        drawn[f"v_{name}"] = jax.random.uniform(key, SHAPES[name], jnp.float32, 0.005, 0.015)
    return drawn


def matmul(a, w):
    return jnp.dot(a, w, preferred_element_type=jnp.float32).astype(jnp.bfloat16)


def normed(h):
    wide = h.astype(jnp.float32)
    scale = lax.rsqrt(jnp.mean(wide**2, -1, keepdims=True) + 1e-6)
    return (wide * scale).astype(jnp.bfloat16)


def layer(h, w):
    a = normed(h)
    gate = jnp.dot(a, w["w_gate"], preferred_element_type=jnp.float32)
    up = jnp.dot(a, w["w_up"], preferred_element_type=jnp.float32)
    return h + matmul((jax.nn.silu(gate) * up).astype(jnp.bfloat16), w["w_down"])


def adamw(w, m, v, g):
    m = 0.9 * m + 0.1 * g
    v = 0.95 * v + 0.05 * g * g
    step = m * lax.rsqrt(v + 1e-8) + 0.1 * w
    return (w - 0.02 * step).astype(jnp.bfloat16), m, v


def stack(weights, h):
    return lax.scan(lambda h, w: (layer(h, w), None), h, weights)[0]


def reference(x, dy, w_gate, w_up, w_down, m_w_gate, m_w_up, m_w_down, v_w_gate, v_w_up, v_w_down):
    weights = dict(zip(NAMES, (w_gate, w_up, w_down), strict=True))

    def take(so_far, sequence):
        h, by_y = sequence
        _, back = jax.vjp(lambda w: stack(w, h), weights)
        return jax.tree.map(lambda total, term: total + term.astype(jnp.float32), so_far, back(by_y)[0]), None

    none_yet = {name: jnp.zeros(w.shape, jnp.float32) for name, w in weights.items()}
    by_weights, _ = lax.scan(take, none_yet, (x, dy))
    gradients = [by_weights[name].astype(jnp.bfloat16).astype(jnp.float32) for name in NAMES]
    new = [
        adamw(w.astype(jnp.float32), m, v, g)
        for w, m, v, g in zip((w_gate, w_up, w_down), (m_w_gate, m_w_up, m_w_down), (v_w_gate, v_w_up, v_w_down), gradients, strict=True)
    ]
    return tuple(one[which] for which in range(3) for one in new)
```

```python
import jax
import jax.numpy as jnp
from jax import lax
from jax.sharding import PartitionSpec as P

NAMES = ("w_gate", "w_up", "w_down")


def matmul(a, w):
    return jnp.dot(a, w, preferred_element_type=jnp.float32).astype(jnp.bfloat16)


def normed(h):
    wide = h.astype(jnp.float32)
    scale = lax.rsqrt(jnp.mean(wide**2, -1, keepdims=True) + 1e-6)
    return (wide * scale).astype(jnp.bfloat16)


def layer(h, w):
    a = normed(h)
    gate = jnp.dot(a, w["w_gate"], preferred_element_type=jnp.float32)
    up = jnp.dot(a, w["w_up"], preferred_element_type=jnp.float32)
    return h + matmul((jax.nn.silu(gate) * up).astype(jnp.bfloat16), w["w_down"])


def adamw(w, m, v, g):
    m = 0.9 * m + 0.1 * g
    v = 0.95 * v + 0.05 * g * g
    step = m * lax.rsqrt(v + 1e-8) + 0.1 * w
    return (w - 0.02 * step).astype(jnp.bfloat16), m, v


def solution(mesh):
    def body(x, dy, *arrays):
        weights, m, v = (arrays[i : i + 3] for i in (0, 3, 6))
        x, dy = x[0], dy[0]
        layers = weights[0].shape[0]
        split = [dict(zip(NAMES, (w[n] for w in weights), strict=True)) for n in range(layers)]

        backs, h = [], x
        for n in range(layers):
            h, back = jax.vjp(layer, h, split[n])
            backs.append(back)
        me = lax.axis_index("dp")
        new = [[None] * layers for _ in NAMES]
        for n in reversed(range(layers)):
            dy, grads = backs[n](dy)
            for k in (2, 0, 1):
                g = lax.psum_scatter(grads[NAMES[k]], "dp", scatter_dimension=0, tiled=True)
                rows = g.shape[0]
                w = lax.dynamic_slice_in_dim(weights[k][n], me * rows, rows)
                w, mm, vv = adamw(w.astype(jnp.float32), m[k][n], v[k][n], g.astype(jnp.float32))
                new[k][n] = (lax.all_gather(w, "dp", axis=0, tiled=True), mm, vv)
        return tuple(jnp.stack([one[which] for one in new[k]]) for which in range(3) for k in range(len(NAMES)))

    whole, rows = P(None, None, None), P(None, "dp", None)
    return jax.shard_map(
        body,
        mesh=mesh,
        in_specs=(P(("rep", "dp")),) * 2 + (whole,) * 3 + (rows,) * 6,
        out_specs=(P("rep"),) * 3 + (P("rep", "dp"),) * 6,
        check_vma=False,
    )
```

```python
import functools
import math

import jax
import jax.numpy as jnp
from jax import lax
from jax.experimental import pallas as pl
from jax.experimental.pallas import tpu as pltpu
from jax.sharding import PartitionSpec as P

BF, F32 = jnp.bfloat16, jnp.float32
MESH = pl.DeviceIdType.MESH
SIDE = 4
KINDS = 4
BLOCKS = 5
LANES = 128
SLOTS = 6
ANY = pl.BlockSpec(memory_space=pl.ANY)


def dot(a, b, da, db):
    return lax.dot_general(a, b, (((da,), (db,)), ((), ())), preferred_element_type=F32)


def normed(wide):
    return (wide * lax.rsqrt(jnp.mean(wide * wide, -1, keepdims=True) + 1e-6)).astype(BF)


def forward_kernel(x_ref, wg_ref, wu_ref, wd_ref, a0_ref, h1_ref, a1_ref, acc, *, rows):
    b = pl.program_id(0)

    def part(t, _):
        at = pl.ds(pl.multiple_of(t * rows, rows), rows)

        @pl.when(b == 0)
        def _():
            a0_ref[at, :] = normed(x_ref[at, :].astype(F32))

        a = a0_ref[at, :]
        gate = dot(a, wg_ref[...], 1, 0)
        up = dot(a, wu_ref[...], 1, 0)
        hidden = (gate * jax.nn.sigmoid(gate) * up).astype(BF)
        more = dot(hidden, wd_ref[...], 1, 0)

        @pl.when(b == 0)
        def _():
            acc[at, :] = more

        @pl.when(b > 0)
        def _():
            acc[at, :] = acc[at, :] + more

        @pl.when(b == pl.num_programs(0) - 1)
        def _():
            h = x_ref[at, :] + acc[at, :].astype(BF)
            h1_ref[at, :] = h
            a1_ref[at, :] = normed(h.astype(F32))

        return 0

    lax.fori_loop(0, x_ref.shape[0] // rows, part, 0)


def first_layer(x, wg, wu, wd):
    n, d = x.shape
    f = wg.shape[2] // BLOCKS
    whole = pl.BlockSpec((n, d), lambda b: (0, 0))
    return pl.pallas_call(
        functools.partial(forward_kernel, rows=256),
        grid=(BLOCKS,),
        out_shape=[jax.ShapeDtypeStruct((n, d), BF)] * 3,
        in_specs=[
            whole,
            pl.BlockSpec((None, d, f), lambda b: (0, 0, b)),
            pl.BlockSpec((None, d, f), lambda b: (0, 0, b)),
            pl.BlockSpec((None, f, d), lambda b: (0, b, 0)),
        ],
        out_specs=[whole] * 3,
        scratch_shapes=[pltpu.VMEM((n, d), F32)],
        compiler_params=pltpu.CompilerParams(vmem_limit_bytes=60 * 2**20),
        name="first_layer",
    )(x, wg, wu, wd)


def step_kernel(a0_h, a1_h, h1_h, dy_h, wg_h, wu_h, wd_h, mg_h, mu_h, md_h, vg_h, vu_h, vd_h,
                og_h, ou_h, od_h, omg_h, omu_h, omd_h, ovg_h, ovu_h, ovd_h, dgs_h, dus_h,
                a, dy, wg, wu, wd, hid, dg, du, acc, dwg, dwd,
                r1, r2, r3, t3, q1, q2, q3,
                cw, cm, cv, nw, nm, nv, ew, em, ev, fw, fm, fv,
                ss, rs, lw, la, lb, ls, lp, lo, *, layers, units, ring, dring):
    n, d = a.shape
    f = wg.shape[1]
    rows_g = d // (SIDE * SIDE)
    rows_d = f * BLOCKS // (SIDE * SIDE)
    sub_g, sub_d = rows_g // KINDS, rows_d // BLOCKS
    per_layer = units // layers
    me = lax.axis_index("dp")
    mx, my = me // SIDE, me % SIDE
    wrap = lambda v: lax.rem(v + 2 * SIDE, SIDE)
    dev = lambda x, y: {"dp": wrap(x) * SIDE + wrap(y)}

    barrier = pltpu.get_barrier_semaphore()
    for x, y in ((mx + 1, my), (mx - 1, my), (mx, my + 1), (mx, my - 1)):
        pl.semaphore_signal(barrier, inc=1, device_id=dev(x, y), device_id_type=MESH)

    def load(src, dst, sem):
        return pltpu.make_async_copy(src, dst, sem)

    def weights(layer, b):
        cols = pl.ds(pl.multiple_of(b * f, LANES), f)
        rows = pl.ds(pl.multiple_of(b * f, 8), f)
        return (load(wg_h.at[layer, :, cols], wg, lw.at[0]), load(wu_h.at[layer, :, cols], wu, lw.at[1]),
                load(wd_h.at[layer, rows, :], wd, lw.at[2]))

    def states(src):
        return load(src, a, la.at[0])

    def saved(b):
        cols = pl.ds(pl.multiple_of(b * f, LANES), f)
        return (load(dg, dgs_h.at[:, cols], ls.at[0]), load(du, dus_h.at[:, cols], ls.at[1]))

    def back(b):
        cols = pl.ds(pl.multiple_of(b * f, LANES), f)
        return (load(dgs_h.at[:, cols], dg, lb.at[0]), load(dus_h.at[:, cols], du, lb.at[1]))

    load_dy = load(dy_h, dy, la.at[1])
    states(a1_h).start()
    load_dy.start()
    for c in weights(layers - 1, 0):
        c.start()
    pl.semaphore_wait(barrier, 4)

    TT = 256

    def tokens(t):
        return pl.ds(pl.multiple_of(t * TT, TT), TT)

    def gradient_columns(which, slot):
        quarter = d // SIDE

        def part(r, _):
            cols = pl.ds(pl.multiple_of(r * quarter, LANES), quarter)
            g = dot(a[:, cols], which[...], 0, 0).astype(BF)
            g = g.reshape(SIDE, KINDS, sub_g, f)
            for i in range(KINDS):
                for c in range(f // LANES):
                    dwg[slot, i, r, :, c * sub_g : (c + 1) * sub_g, :] = g[:, i, :, c * LANES : (c + 1) * LANES]
            return 0

        lax.fori_loop(0, SIDE, part, 0)

    def gradient_rows(b, first):
        cols_k = d // KINDS

        def part(i, _):
            cols = pl.ds(pl.multiple_of(i * cols_k, LANES), cols_k)
            g = dot(hid[...], dy[:, cols], 0, 0).astype(BF)
            for k in range(f // sub_d):
                unit = b * (f // sub_d) + k
                owner, j = unit // BLOCKS, unit % BLOCKS
                slot = lax.rem(first + j, dring)
                for c in range(cols_k // LANES):
                    dwd[slot, i, owner // SIDE, owner % SIDE, c * sub_d : (c + 1) * sub_d, :] = (
                        g[k * sub_d : (k + 1) * sub_d, c * LANES : (c + 1) * LANES])
            return 0

        lax.fori_loop(0, KINDS, part, 0)

    def hidden_block(layer, b, slot):
        for c in weights(layer, b):
            c.wait()

        @pl.when(b == 0)
        def _():
            states(a0_h).wait()

            @pl.when(layer == layers - 1)
            def _():
                load_dy.wait()

        def part(t, _):
            at = tokens(t)
            gate = dot(a[at, :], wg[...], 1, 0)
            up = dot(a[at, :], wu[...], 1, 0)
            back = dot(dy[at, :], wd[...], 1, 1).astype(BF).astype(F32)
            s = jax.nn.sigmoid(gate)
            silu = gate * s
            hid[at, :] = (silu * up).astype(BF)
            du[at, :] = (back * silu).astype(BF)
            dg[at, :] = (back * up * (s + silu * (1 - s))).astype(BF)
            return 0

        lax.fori_loop(0, n // TT, part, 0)

        @pl.when(layer > 0)
        def _():
            for c in saved(b):
                c.start()

        @pl.when(b < BLOCKS - 1)
        def _():
            for c in weights(layer, b + 1):
                c.start()

        @pl.when((b == BLOCKS - 1) & (layer > 0))
        def _():
            for c in weights(layer, 0)[:2]:
                c.start()

        gradient_columns(dg, slot)

    def hidden_rest(layer, b, slot, first):
        gradient_columns(du, slot)
        gradient_rows(b, first)

        @pl.when(layer > 0)
        def _():
            for c in saved(b):
                c.wait()

            @pl.when(b == BLOCKS - 1)
            def _():
                for c in back(0):
                    c.start()
                states(h1_h).start()

    def states_back(layer, q):
        for c in weights(layer, q)[:2]:
            c.wait()
        for c in back(q):
            c.wait()

        def part(t, _):
            at = tokens(t)
            more = dot(dg[at, :], wg[...], 1, 1) + dot(du[at, :], wu[...], 1, 1)

            @pl.when(q == 0)
            def _():
                acc[at, :] = more

            @pl.when(q > 0)
            def _():
                acc[at, :] = acc[at, :] + more

            return 0

        lax.fori_loop(0, n // TT, part, 0)

        @pl.when(q < BLOCKS - 1)
        def _():
            for c in weights(layer, q + 1)[:2]:
                c.start()
            for c in back(q + 1):
                c.start()

        @pl.when(q == BLOCKS - 1)
        def _():
            for c in weights(layer - 1, 0):
                c.start()
            states(h1_h).wait()

            def part(t, _):
                at = pl.ds(pl.multiple_of(t * 64, 64), 64)
                wide = a[at, :].astype(F32)
                scale = lax.rsqrt(jnp.mean(wide * wide, -1, keepdims=True) + 1e-6)
                by = acc[at, :].astype(BF).astype(F32)
                along = jnp.mean(by * wide, -1, keepdims=True)
                more = by * scale - wide * (scale * scale * scale * along)
                dy[at, :] = (dy[at, :].astype(F32) + more.astype(BF).astype(F32)).astype(BF)
                return 0

            lax.fori_loop(0, n // 64, part, 0)
            states(a0_h).start()

    def place(u):
        layer = layers - 1 - u // per_layer
        k = lax.rem(u, per_layer)
        down = k >= 2 * BLOCKS
        return layer, jnp.where(down, 2, lax.rem(k, 2)), jnp.where(down, k - 2 * BLOCKS, k // 2), k

    def dring_slot(u):
        return lax.rem((u // per_layer) * BLOCKS + lax.rem(u, per_layer) - 2 * BLOCKS + dring, dring)

    def steps(i):
        s = 1 - 2 * (i % 2)
        xs, ys = (dev(mx + s, my), dev(mx - s, my)), (dev(mx, my + s), dev(mx, my - s))
        return (*xs, *ys, mx, my, s) if i < 2 else (*ys, *xs, my, mx, s)

    def rcopy(src, dst, u, i, k, to):
        n_ = lax.rem(u, SLOTS)
        return pltpu.make_async_remote_copy(
            src_ref=src, dst_ref=dst, send_sem=ss.at[n_, i, k], recv_sem=rs.at[n_, i, k], device_id=to, device_id_type=MESH)

    def own(u, i, p):
        g, dn = dwg.at[lax.rem(u, ring), i], dwd.at[dring_slot(u), i]
        return tuple(w.at[p] if i < 2 else w.at[:, p] for w in (g, dn))

    def on_own(u, do):
        k = lax.rem(u, per_layer)
        pl.when(k < 2 * BLOCKS)(lambda: do(0))
        pl.when(k >= 2 * BLOCKS)(lambda: do(1))

    def s0_copies(u, i, which):
        ahead, behind, _, _, pf, _, s = steps(i)
        n_ = lax.rem(u, SLOTS)
        return (rcopy(own(u, i, wrap(pf + 2))[which], r1.at[n_, i], u, i, 0, ahead),
                rcopy(own(u, i, wrap(pf - s))[which], r2.at[n_, i], u, i, 1, behind))

    def s1_copy(u, i):
        ahead = steps(i)[0]
        n_ = lax.rem(u, SLOTS)
        return rcopy(r1.at[n_, i], r3.at[n_, i], u, i, 2, ahead)

    def s2_copies(u, i):
        _, _, ahead, behind, _, ps, s = steps(i)
        n_ = lax.rem(u, SLOTS)
        return (rcopy(r3.at[n_, i, wrap(ps + 2)], q1.at[n_, i], u, i, 3, ahead),
                rcopy(r3.at[n_, i, wrap(ps - s)], q2.at[n_, i], u, i, 4, behind))

    def s3_copy(u, i):
        ahead = steps(i)[2]
        n_ = lax.rem(u, SLOTS)
        return rcopy(q1.at[n_, i], q3.at[n_, i], u, i, 5, ahead)

    def state_copies(u):
        layer, _, j, _ = place(u)
        z = lax.rem(u, 2)
        cols = pl.ds(pl.multiple_of(j * f, LANES), f)
        rows = pl.ds(pl.multiple_of(me * rows_d + j * sub_d, 8), sub_d)
        mine = pl.ds(pl.multiple_of(j * sub_d, 8), sub_d)
        first = pl.ds(pl.multiple_of(me * rows_g, 8), rows_g)
        ins = tuple(
            (load(w.at[layer, first, cols], cw.at[z], lp.at[z, 0]), load(m.at[layer, :, cols], cm.at[z], lp.at[z, 1]),
             load(v.at[layer, :, cols], cv.at[z], lp.at[z, 2]))
            for w, m, v in ((wg_h, mg_h, vg_h), (wu_h, mu_h, vu_h))
        ) + ((load(wd_h.at[layer, rows, :], ew.at[z], lp.at[z, 0]), load(md_h.at[layer, mine, :], em.at[z], lp.at[z, 1]),
              load(vd_h.at[layer, mine, :], ev.at[z], lp.at[z, 2])),)
        outs = tuple(
            (load(nw.at[z], w.at[layer, mx, my, :, cols], lo.at[z, 0]), load(nm.at[z], m.at[layer, :, cols], lo.at[z, 1]),
             load(nv.at[z], v.at[layer, :, cols], lo.at[z, 2]))
            for w, m, v in ((og_h, omg_h, ovg_h), (ou_h, omu_h, ovu_h))
        ) + ((load(fw.at[z], od_h.at[layer, mx, my, mine, :], lo.at[z, 0]), load(fm.at[z], omd_h.at[layer, mine, :], lo.at[z, 1]),
              load(fv.at[z], ovd_h.at[layer, mine, :], lo.at[z, 2])),)
        return ins, outs

    def on_matrix(u, do):
        k = lax.rem(u, per_layer)
        down = k >= 2 * BLOCKS
        for which, test in enumerate((~down & (lax.rem(k, 2) == 0), ~down & (lax.rem(k, 2) == 1), down)):
            pl.when(test)(functools.partial(do, which))

    def out_at(u, i, which):
        layer, _, j, _ = place(u)
        if which < 2:
            cols = pl.ds(pl.multiple_of(j * f, LANES), f)
            return lambda x, y: (og_h, ou_h)[which].at[layer, x, y, pl.ds(i * sub_g, sub_g), cols]
        rows = pl.ds(pl.multiple_of(j * sub_d, 8), sub_d)
        wide = d // KINDS
        return lambda x, y: od_h.at[layer, x, y, rows, pl.ds(i * wide, wide)]

    def new_block(u, i, which):
        z = lax.rem(u, 2)
        wide = d // KINDS
        return nw.at[z, pl.ds(i * sub_g, sub_g), :] if which < 2 else fw.at[z, :, pl.ds(i * wide, wide)]

    def s4_copies(u, i, which):
        _, _, ahead, behind, _, _, _ = steps(i)
        dst = out_at(u, i, which)(mx, my)
        src = new_block(u, i, which)
        return (rcopy(src, dst, u, i, 6, ahead), rcopy(src, dst, u, i, 7, behind))

    def s5_copy(u, i, which):
        _, _, ahead, _, pf, ps, s = steps(i)
        at = out_at(u, i, which)
        src = at(pf, wrap(ps - s)) if i < 2 else at(wrap(ps - s), pf)
        return rcopy(src, src, u, i, 8, ahead)

    every = pl.ds(0, SIDE)

    def s6_copies(u, i, which):
        ahead, behind, _, _, pf, _, _ = steps(i)
        at = out_at(u, i, which)
        src = at(pf, every) if i < 2 else at(every, pf)
        return (rcopy(src, src, u, i, 9, ahead), rcopy(src, src, u, i, 10, behind))

    def s7_copy(u, i, which):
        ahead, _, _, _, pf, _, s = steps(i)
        at = out_at(u, i, which)
        p = wrap(pf - s)
        src = at(p, every) if i < 2 else at(every, p)
        return rcopy(src, src, u, i, 11, ahead)

    def stage0(u):
        def do(which):
            for i in range(KINDS):
                for c in s0_copies(u, i, which):
                    c.start()
        on_own(u, do)

    def stage1(u):
        n_ = lax.rem(u, SLOTS)

        def do(which):
            for i in range(KINDS):
                _, _, _, _, pf, _, s = steps(i)
                s0_copies(u, i, which)[0].wait()
                mine = own(u, i, wrap(pf + s))[which]
                r1[n_, i] = (r1[n_, i].astype(F32) + mine[...].astype(F32)).astype(BF)
                s1_copy(u, i).start()
        on_own(u, do)

    def stage2(u):
        n_ = lax.rem(u, SLOTS)

        def do(which):
            for i in range(KINDS):
                _, _, _, _, pf, ps, s = steps(i)
                s0_copies(u, i, which)[1].wait()
                s1_copy(u, i).wait()
                mine = own(u, i, pf)[which]
                for k in (2, -s, s, 0):
                    p = wrap(ps + k)
                    total = r2[n_, i, p].astype(F32) + r3[n_, i, p].astype(F32) + mine[p].astype(F32)
                    if k in (2, -s):
                        r3[n_, i, p] = total.astype(BF)
                    else:
                        t3[n_, i, 0 if k else 1] = total
                for c in s2_copies(u, i):
                    c.start()
        on_own(u, do)

    def stage3(u):
        n_ = lax.rem(u, SLOTS)

        def begin(which):
            for c in state_copies(u)[0][which]:
                c.start()
        on_matrix(u, begin)
        for i in range(KINDS):
            s2_copies(u, i)[0].wait()
            q1[n_, i] = (q1[n_, i].astype(F32) + t3[n_, i, 0]).astype(BF)
            s3_copy(u, i).start()

    def stage4(u):
        n_, z = lax.rem(u, SLOTS), lax.rem(u, 2)

        def update(g, w, m, v):
            g = g.astype(BF).astype(F32)
            m = 0.9 * m + 0.1 * g
            v = 0.95 * v + 0.05 * g * g
            w = w.astype(F32)
            return (w - 0.02 * (m * lax.rsqrt(v + 1e-8) + 0.1 * w)).astype(BF), m, v

        for i in range(KINDS):
            s2_copies(u, i)[1].wait()
            s3_copy(u, i).wait()

        def do(which):
            for c in state_copies(u)[0][which]:
                c.wait()
            wide, sub = d // KINDS, sub_g if which < 2 else sub_d
            for i in range(KINDS):
                for c in range(r1.shape[3] // sub):
                    part = pl.ds(c * sub, sub)
                    g = q2[n_, i, part, :].astype(F32) + q3[n_, i, part, :].astype(F32) + t3[n_, i, 1, part, :]
                    if which < 2:
                        at = (z, pl.ds(i * sub, sub), pl.ds(c * LANES, LANES))
                        nw[at], nm[at], nv[at] = update(g, cw[at], cm[at], cv[at])
                    else:
                        at = (z, slice(None), pl.ds(i * wide + c * LANES, LANES))
                        fw[at], fm[at], fv[at] = update(g, ew[at], em[at], ev[at])
                for c in s4_copies(u, i, which):
                    c.start()
            for c in state_copies(u)[1][which]:
                c.start()
        on_matrix(u, do)

    def stage5(u):
        def do(which):
            for c in state_copies(u)[1][which]:
                c.wait()
            for i in range(KINDS):
                for c in s4_copies(u, i, which):
                    c.wait()
                s5_copy(u, i, which).start()
        on_matrix(u, do)

    def stage6(u):
        def do(which):
            for i in range(KINDS):
                s5_copy(u, i, which).wait()
                for c in s6_copies(u, i, which):
                    c.start()
        on_matrix(u, do)

    def stage7(u):
        def do(which):
            for i in range(KINDS):
                for c in s6_copies(u, i, which):
                    c.wait()
                s7_copy(u, i, which).start()
        on_matrix(u, do)

    def stage8(u):
        def do(which):
            for i in range(KINDS):
                s7_copy(u, i, which).wait()
        on_matrix(u, do)

    stages = (stage0, stage1, stage2, stage3, stage4, stage5, stage6, stage7, stage8)

    def tick(t, _):
        for k, stage in enumerate(stages):
            u = t - 1 - k
            pl.when((u >= 0) & (u < units))(functools.partial(stage, u))

        layer, _, j, k = place(t)
        busy = t < units
        even = lax.rem(k, 2) == 0
        pl.when(busy & (k < 2 * BLOCKS) & even)(lambda: hidden_block(layer, j, lax.rem(t, ring)))
        pl.when(busy & (k < 2 * BLOCKS) & ~even)(
            lambda: hidden_rest(layer, j, lax.rem(t, ring), (layers - 1 - layer) * BLOCKS))
        pl.when(busy & (k >= 2 * BLOCKS) & (layer > 0))(lambda: states_back(layer, j))
        return 0

    lax.fori_loop(0, units + len(stages), tick, 0)


def train_step(layers, a0, a1, h1, dy, ws, ms, vs):
    n, d = dy.shape
    f = ws[0].shape[2] // BLOCKS
    owners = SIDE * SIDE
    rows_g, rows_d = d // owners, f * BLOCKS // owners
    units = layers * 3 * BLOCKS
    ring, dring = 4, 7
    flat = rows_g * f // KINDS // LANES
    blocks = (SLOTS, KINDS, SIDE, flat, LANES)
    block = (SLOTS, KINDS, flat, LANES)
    gate, down = (2, rows_g, f), (2, rows_d // BLOCKS, d)
    vmem, dma = pltpu.VMEM, pltpu.SemaphoreType.DMA
    sd = jax.ShapeDtypeStruct
    outs = pl.pallas_call(
        functools.partial(step_kernel, layers=layers, units=units, ring=ring, dring=dring),
        out_shape=[sd((layers, SIDE, SIDE, rows_g, d and f * BLOCKS), BF)] * 2
        + [sd((layers, SIDE, SIDE, rows_d, d), BF)]
        + [sd(m.shape, F32) for m in ms] + [sd(v.shape, F32) for v in vs]
        + [sd((n, f * BLOCKS), BF)] * 2,
        in_specs=[ANY] * 13,
        out_specs=[ANY] * 11,
        scratch_shapes=[
            vmem((n, d), BF), vmem((n, d), BF), vmem((d, f), BF), vmem((d, f), BF), vmem((f, d), BF),
            vmem((n, f), BF), vmem((n, f), BF), vmem((n, f), BF), vmem((n, d), F32),
            vmem((ring, KINDS, SIDE, SIDE, flat, LANES), BF), vmem((dring, KINDS, SIDE, SIDE, flat, LANES), BF),
            vmem(blocks, BF), vmem(blocks, BF), vmem(blocks, BF), vmem((SLOTS, KINDS, 2, flat, LANES), F32),
            vmem(block, BF), vmem(block, BF), vmem(block, BF),
            vmem(gate, BF), vmem(gate, F32), vmem(gate, F32), vmem(gate, BF), vmem(gate, F32), vmem(gate, F32),
            vmem(down, BF), vmem(down, F32), vmem(down, F32), vmem(down, BF), vmem(down, F32), vmem(down, F32),
            dma((SLOTS, KINDS, 12)), dma((SLOTS, KINDS, 12)),
            dma((3,)), dma((2,)), dma((2,)), dma((2,)), dma((2, 3)), dma((2, 3)),
        ],
        compiler_params=pltpu.CompilerParams(collective_id=0, has_side_effects=True, vmem_limit_bytes=67043328),
        name="train_step",
    )(a0, a1, h1, dy, *ws, *ms, *vs)
    return outs[:9]


def solution(mesh):
    assert mesh.shape["dp"] == SIDE * SIDE

    def body(x, dy, *arrays):
        ws, ms, vs = (arrays[i : i + 3] for i in (0, 3, 6))
        x, dy = x[0], dy[0]
        a0, h1, a1 = first_layer(x, *ws)
        outs = train_step(ws[0].shape[0], a0, a1, h1, dy, ws, ms, vs)
        return tuple(o.reshape(w.shape) for o, w in zip(outs[:3], ws, strict=True)) + tuple(outs[3:])

    whole, rows = P(None, None, None), P(None, "dp", None)
    return jax.shard_map(
        body,
        mesh=mesh,
        in_specs=(P(("rep", "dp")),) * 2 + (whole,) * 3 + (rows,) * 6,
        out_specs=(P("rep"),) * 3 + (P("rep", "dp"),) * 6,
        check_vma=False,
    )
```

```python
import functools

import jax
import jax.numpy as jnp
from jax import lax
from jax.experimental import pallas as pl
from jax.experimental.pallas import tpu as pltpu
from jax.sharding import PartitionSpec as P

BF, F32 = jnp.bfloat16, jnp.float32
MESH = pl.DeviceIdType.MESH
SIDE = 4
KINDS = 4
BLOCKS = 5
LANES = 128
SPLIT = 1
WHEN = (0, 1, 2, 3, 4, 5, 7, 8, 9)
UNROLL = 4
VLIM = 38 * 2**20
SLOTS = 4
ANY = pl.BlockSpec(memory_space=pl.ANY)


def dot(a, b, da, db):
    return lax.dot_general(a, b, (((da,), (db,)), ((), ())), preferred_element_type=F32)


def normed(wide):
    return (wide * lax.rsqrt(jnp.mean(wide * wide, -1, keepdims=True) + 1e-6)).astype(BF)


def step_kernel(x_h, dy_h, wg_h, wu_h, wd_h, mg_h, mu_h, md_h, vg_h, vu_h, vd_h,
                og_h, ou_h, od_h, omg_h, omu_h, omd_h, ovg_h, ovu_h, ovd_h, both_h, a, h, dy, wgu, hid, both,
                wd, acc, dwg, dwd,
                r1, r2, r3, t3, q1, q2, q3,
                cw, cm, cv, nw, nm, nv, ew, em, ev, fw, fm, fv,
                ss, rs, lw, la, lb, ls, lp, lo, lf, *, layers, units, ring):
    n, d = a.shape
    f = wd.shape[1]
    rows_g = d // (SIDE * SIDE)
    rows_d = f * BLOCKS // (SIDE * SIDE)
    sub_g, sub_d = rows_g // KINDS, rows_d // BLOCKS
    per_layer = units // layers
    me = lax.axis_index("dp")
    mx, my = me // SIDE, me % SIDE
    wrap = lambda v: lax.rem(v + 2 * SIDE, SIDE)
    dev = lambda x, y: {"dp": wrap(x) * SIDE + wrap(y)}

    barrier = pltpu.get_barrier_semaphore()
    for x, y in ((mx + 1, my), (mx - 1, my), (mx, my + 1), (mx, my - 1)):
        pl.semaphore_signal(barrier, inc=1, device_id=dev(x, y), device_id_type=MESH)

    load = lambda src, dst, sem: lambda: pltpu.make_async_copy(src, dst, sem)

    def start(*copies):
        for c in copies:
            c().start()

    def wait(*copies):
        for c in copies:
            c().wait()

    def weights(w):
        z, b, turn = lax.rem(w, 2), lax.rem(w, BLOCKS), w // BLOCKS
        layer = jnp.where((turn == 0) | (turn == 3), 0, layers - 1)
        cols = pl.ds(pl.multiple_of(b * f, LANES), f)
        rows = pl.ds(pl.multiple_of(b * f, 8), f)
        return (load(wg_h.at[layer, :, cols], wgu.at[z, :, pl.ds(0, f)], lw.at[z, 0]),
                load(wu_h.at[layer, :, cols], wgu.at[z, :, pl.ds(f, f)], lw.at[z, 1]),
                load(wd_h.at[layer, rows, :], wd.at[z], lw.at[z, 2]))

    def next_weights(w):
        wait(*weights(w))
        pl.when(w < 4 * BLOCKS - 1)(lambda: start(*weights(w + 1)))

    saved = lambda b: load(both, both_h.at[b], ls)
    back = lambda b: load(both_h.at[b], both, lb.at[0])
    TILE, NORM = 256, 64
    load_x = [load(x_h.at[pl.ds(t * TILE, TILE), :], h.at[pl.ds(t * TILE, TILE), :], la.at[t]) for t in range(n // TILE)]
    load_dy = load(dy_h, dy, lb.at[1])
    start(load_x[0], *weights(0), *load_x[1:])

    def tokens(t, size=TILE):
        return pl.ds(pl.multiple_of(t * size, size), size)

    def loop(count, do, unroll):
        def some(t, _):
            for k in range(unroll):
                do(t * unroll + k)
            return 0

        lax.fori_loop(0, count // unroll, some, 0)

    def every_token(do, size=NORM, unroll=1):
        loop(n // size, lambda t: do(tokens(t, size)), unroll)

    def norm_states(at):
        a[at, :] = normed(h[at, :].astype(F32))

    def first_units(b):
        z = lax.rem(b, 2)
        at_start, at_end = isinstance(b, int) and b == 0, isinstance(b, int) and b == BLOCKS - 1
        next_weights(b)

        def do(t):
            at = tokens(t)
            if at_start:
                pltpu.make_async_copy(x_h.at[at, :], h.at[at, :], la.at[t]).wait()
                norm_states(at)
            gu = dot(a[at, :], wgu[z], 1, 0)
            gate, up = gu[:, :f], gu[:, f:]
            hidden = (gate * jax.nn.sigmoid(gate) * up).astype(BF)
            more = dot(hidden, wd[z], 1, 0)
            if at_end:
                new = h[at, :] + (acc[at, :] + more).astype(BF)
                h[at, :] = new
                a[at, :] = normed(new.astype(F32))
            else:
                acc[at, :] = more if at_start else acc[at, :] + more

        loop(n // TILE, do, UNROLL)

    def clear(at):
        acc[at, :] = jnp.zeros((NORM, d), F32)

    def hidden_units(layer, b, piece):
        w = jnp.where(layer > 0, BLOCKS, 3 * BLOCKS) + b
        z = lax.rem(w, 2)

        @pl.when(piece == 0)
        def _():
            next_weights(w)

            @pl.when((b == 0) & (layer == 0))
            def _():
                wait(*load_x)
                every_token(norm_states)

            @pl.when((b == 0) & (layer > 0))
            def _():
                wait(load_dy)

        def part(t):
            at = tokens(piece * (n // TILE // (2 * SPLIT)) + t)
            gu = dot(a[at, :], wgu[z], 1, 0)
            gate, up = gu[:, :f], gu[:, f:]
            back = dot(dy[at, :], wd[z], 1, 1).astype(BF).astype(F32)
            s = jax.nn.sigmoid(gate)
            silu = gate * s
            hid[at, :] = (silu * up).astype(BF)
            both[at, f:] = (back * silu).astype(BF)
            both[at, :f] = (back * up * (s + silu * (1 - s))).astype(BF)

        loop(n // TILE // (2 * SPLIT), part, UNROLL)
        pl.when((piece == 2 * SPLIT - 1) & (layer > 0))(lambda: start(saved(b)))

    def gradient_columns(u, piece):
        quarter = d // SIDE

        def part(r):
            r = piece * (SIDE // SPLIT) + r
            cols = pl.ds(pl.multiple_of(r * quarter, LANES), quarter)
            g = dot(a[:, cols], both[...], 0, 0).astype(BF)
            g = g.reshape(SIDE, KINDS, sub_g, 2 * f)
            for which in range(2):
                slot = lax.rem(u + which, ring)
                for i in range(KINDS):
                    for c in range(f // LANES):
                        at = which * f + c * LANES
                        dwg[slot, i, r, :, c * sub_g : (c + 1) * sub_g, :] = g[:, i, :, at : at + LANES]

        loop(SIDE // SPLIT, part, UNROLL)

    def gradient_rows(layer, b, piece):
        cols_k = d // KINDS

        def part(i):
            i = piece * (KINDS // SPLIT) + i
            cols = pl.ds(pl.multiple_of(i * cols_k, LANES), cols_k)
            g = dot(hid[...], dy[:, cols], 0, 0).astype(BF)
            for k in range(f // sub_d):
                unit = b * (f // sub_d) + k
                owner, j = unit // BLOCKS, unit % BLOCKS
                slot = lax.rem((layers - 1 - layer) * BLOCKS + j, dwd.shape[0])
                for c in range(cols_k // LANES):
                    dwd[slot, i, owner // SIDE, owner % SIDE, c * sub_d : (c + 1) * sub_d, :] = (
                        g[k * sub_d : (k + 1) * sub_d, c * LANES : (c + 1) * LANES])

        loop(KINDS // SPLIT, part, UNROLL)

        @pl.when((layer > 0) & (piece == SPLIT - 1))
        def _():
            wait(saved(b))
            pl.when(b == BLOCKS - 1)(lambda: start(back(0)))

    def states_back(q, piece):
        w = 2 * BLOCKS + q
        z = lax.rem(w, 2)

        @pl.when(piece == 0)
        def _():
            pl.when(q == 0)(lambda: every_token(clear))
            next_weights(w)
            wait(back(q))

        def part(t):
            at = tokens(piece * (n // TILE // (2 * SPLIT)) + t)
            acc[at, :] = acc[at, :] + dot(both[at, :], wgu[z], 1, 1)

        loop(n // TILE // (2 * SPLIT), part, UNROLL)
        pl.when((piece == 2 * SPLIT - 1) & (q < BLOCKS - 1))(lambda: start(back(q + 1)))

        @pl.when((piece == 2 * SPLIT - 1) & (q == BLOCKS - 1))
        def _():
            def do(at):
                wide = h[at, :].astype(F32)
                scale = lax.rsqrt(jnp.mean(wide * wide, -1, keepdims=True) + 1e-6)
                by = acc[at, :].astype(BF).astype(F32)
                along = jnp.mean(by * wide, -1, keepdims=True)
                more = by * scale - wide * (scale * scale * scale * along)
                dy[at, :] = (dy[at, :].astype(F32) + more.astype(BF).astype(F32)).astype(BF)

            every_token(do)
            start(*load_x)

    def place(u):
        k = lax.rem(u, per_layer)
        return layers - 1 - u // per_layer, jnp.where(k >= 2 * BLOCKS, k - 2 * BLOCKS, k // 2)

    def steps(i):
        s = 1 - 2 * (i % 2)
        xs, ys = (dev(mx + s, my), dev(mx - s, my)), (dev(mx, my + s), dev(mx, my - s))
        return (*xs, *ys, mx, my, s) if i < 2 else (*ys, *xs, my, mx, s)

    def rcopy(src, dst, u, i, k, to):
        n_ = lax.rem(u, SLOTS)
        return lambda: pltpu.make_async_remote_copy(
            src_ref=src, dst_ref=dst, send_sem=ss.at[n_, i, k], recv_sem=rs.at[n_, i, k], device_id=to, device_id_type=MESH)

    def own(u, i, p, which):
        w = dwd.at[lax.rem(u // per_layer * BLOCKS + place(u)[1], dwd.shape[0]), i] if which else dwg.at[lax.rem(u, ring), i]
        return w.at[p] if i < 2 else w.at[:, p]

    def on_own(u, do):
        k = lax.rem(u, per_layer)
        pl.when(k < 2 * BLOCKS)(lambda: do(0))
        pl.when(k >= 2 * BLOCKS)(lambda: do(1))

    def s0_copies(u, i, which):
        ahead, behind, _, _, pf, _, s = steps(i)
        n_ = lax.rem(u, SLOTS)
        return (rcopy(own(u, i, wrap(pf + 2), which), r1.at[n_, i], u, i, 0, ahead),
                rcopy(own(u, i, wrap(pf - s), which), r2.at[n_, i], u, i, 1, behind))

    def s1_copy(u, i):
        n_ = lax.rem(u, SLOTS)
        return rcopy(r1.at[n_, i], r3.at[n_, i], u, i, 2, steps(i)[0])

    def s2_copies(u, i):
        _, _, ahead, behind, _, ps, s = steps(i)
        n_ = lax.rem(u, SLOTS)
        return (rcopy(r3.at[n_, i, wrap(ps + 2)], q1.at[n_, i], u, i, 3, ahead),
                rcopy(r3.at[n_, i, wrap(ps - s)], q2.at[n_, i], u, i, 4, behind))

    def s3_copy(u, i):
        n_ = lax.rem(u, SLOTS)
        return rcopy(q1.at[n_, i], q3.at[n_, i], u, i, 5, steps(i)[2])

    def state_copies(u, which, out):
        layer, j = place(u)
        z = lax.rem(u, 2)
        cols = pl.ds(pl.multiple_of(j * f, LANES), f)
        rows = pl.ds(pl.multiple_of(me * rows_d + j * sub_d, 8), sub_d)
        mine = pl.ds(pl.multiple_of(j * sub_d, 8), sub_d)
        first = pl.ds(pl.multiple_of(me * rows_g, 8), rows_g)
        if which < 2:
            if out:
                w, m, v = ((og_h, omg_h, ovg_h), (ou_h, omu_h, ovu_h))[which]
                return (load(nw.at[z], w.at[layer, mx, my, :, cols], lo.at[z, 0]), load(nm.at[z], m.at[layer, :, cols], lo.at[z, 1]),
                        load(nv.at[z], v.at[layer, :, cols], lo.at[z, 2]))
            w, m, v = ((wg_h, mg_h, vg_h), (wu_h, mu_h, vu_h))[which]
            return (load(w.at[layer, first, cols], cw.at[z], lp.at[z, 0]), load(m.at[layer, :, cols], cm.at[z], lp.at[z, 1]),
                    load(v.at[layer, :, cols], cv.at[z], lp.at[z, 2]))
        if out:
            return (load(fw.at[z], od_h.at[layer, mx, my, mine, :], lo.at[z, 0]), load(fm.at[z], omd_h.at[layer, mine, :], lo.at[z, 1]),
                    load(fv.at[z], ovd_h.at[layer, mine, :], lo.at[z, 2]))
        return (load(wd_h.at[layer, rows, :], ew.at[z], lp.at[z, 0]), load(md_h.at[layer, mine, :], em.at[z], lp.at[z, 1]),
                load(vd_h.at[layer, mine, :], ev.at[z], lp.at[z, 2]))

    def on_matrix(u, do):
        k = lax.rem(u, per_layer)
        down = k >= 2 * BLOCKS
        for which, test in enumerate((~down & (lax.rem(k, 2) == 0), ~down & (lax.rem(k, 2) == 1), down)):
            pl.when(test)(functools.partial(do, which))

    def out_at(u, i, which):
        layer, j = place(u)
        if which < 2:
            cols = pl.ds(pl.multiple_of(j * f, LANES), f)
            return lambda x, y: (og_h, ou_h)[which].at[layer, x, y, pl.ds(i * sub_g, sub_g), cols]
        rows = pl.ds(pl.multiple_of(j * sub_d, 8), sub_d)
        wide = d // KINDS
        return lambda x, y: od_h.at[layer, x, y, rows, pl.ds(i * wide, wide)]

    def s4_copies(u, i, which):
        _, _, ahead, behind, _, _, _ = steps(i)
        z = lax.rem(u, 2)
        wide = d // KINDS
        dst = out_at(u, i, which)(mx, my)
        src = nw.at[z, pl.ds(i * sub_g, sub_g), :] if which < 2 else fw.at[z, :, pl.ds(i * wide, wide)]
        return (rcopy(src, dst, u, i, 6, ahead), rcopy(src, dst, u, i, 7, behind))

    def s5_copy(u, i, which):
        _, _, ahead, _, pf, ps, s = steps(i)
        at = out_at(u, i, which)
        src = at(pf, wrap(ps - s)) if i < 2 else at(wrap(ps - s), pf)
        return rcopy(src, src, u, i, 8, ahead)

    every = pl.ds(0, SIDE)

    def s6_copies(u, i, which):
        ahead, behind, _, _, pf, _, _ = steps(i)
        at = out_at(u, i, which)
        src = at(pf, every) if i < 2 else at(every, pf)
        return (rcopy(src, src, u, i, 9, ahead), rcopy(src, src, u, i, 10, behind))

    def s7_copy(u, i, which):
        ahead, _, _, _, pf, _, s = steps(i)
        at = out_at(u, i, which)
        p = wrap(pf - s)
        src = at(p, every) if i < 2 else at(every, p)
        return rcopy(src, src, u, i, 11, ahead)

    def stage0(u):
        def do(which):
            for i in range(KINDS):
                start(*s0_copies(u, i, which))
        on_own(u, do)

    def stage1(u):
        n_ = lax.rem(u, SLOTS)

        def do(which):
            for i in range(KINDS):
                _, _, _, _, pf, _, s = steps(i)
                wait(s0_copies(u, i, which)[0])
                mine = own(u, i, wrap(pf + s), which)
                r1[n_, i] = (r1[n_, i].astype(F32) + mine[...].astype(F32)).astype(BF)
                start(s1_copy(u, i))
        on_own(u, do)

    def stage2(u):
        n_ = lax.rem(u, SLOTS)

        def do(which):
            for i in range(KINDS):
                _, _, _, _, pf, ps, s = steps(i)
                wait(s0_copies(u, i, which)[1], s1_copy(u, i))
                mine = own(u, i, pf, which)
                for k in (2, -s, s, 0):
                    p = wrap(ps + k)
                    total = r2[n_, i, p].astype(F32) + r3[n_, i, p].astype(F32) + mine[p].astype(F32)
                    if k in (2, -s):
                        r3[n_, i, p] = total.astype(BF)
                    else:
                        t3[n_, i, 0 if k else 1] = total
                start(*s2_copies(u, i))
        on_own(u, do)

    def stage3(u):
        n_ = lax.rem(u, SLOTS)
        on_matrix(u, lambda which: start(*state_copies(u, which, False)))
        for i in range(KINDS):
            wait(s2_copies(u, i)[0])
            q1[n_, i] = (q1[n_, i].astype(F32) + t3[n_, i, 0]).astype(BF)
            start(s3_copy(u, i))

    def stage4(u):
        n_, z = lax.rem(u, SLOTS), lax.rem(u, 2)

        def update(g, w, m, v):
            g = g.astype(BF).astype(F32)
            m = 0.9 * m + 0.1 * g
            v = 0.95 * v + 0.05 * g * g
            w = w.astype(F32)
            return (w - 0.02 * (m * lax.rsqrt(v + 1e-8) + 0.1 * w)).astype(BF), m, v

        for i in range(KINDS):
            wait(s2_copies(u, i)[1], s3_copy(u, i))

        def do(which):
            wait(*state_copies(u, which, False))
            wide, sub = d // KINDS, sub_g if which < 2 else sub_d
            for i in range(KINDS):
                for c in range(r1.shape[3] // sub):
                    part = pl.ds(c * sub, sub)
                    g = q2[n_, i, part, :].astype(F32) + q3[n_, i, part, :].astype(F32) + t3[n_, i, 1, part, :]
                    if which < 2:
                        at = (z, pl.ds(i * sub, sub), pl.ds(c * LANES, LANES))
                        nw[at], nm[at], nv[at] = update(g, cw[at], cm[at], cv[at])
                    else:
                        at = (z, slice(None), pl.ds(i * wide + c * LANES, LANES))
                        fw[at], fm[at], fv[at] = update(g, ew[at], em[at], ev[at])
                start(*s4_copies(u, i, which))
            start(*state_copies(u, which, True))
        on_matrix(u, do)

    def stage5(u):
        def do(which):
            wait(*state_copies(u, which, True))
            for i in range(KINDS):
                wait(*s4_copies(u, i, which))
                start(s5_copy(u, i, which))
        on_matrix(u, do)

    def stage6(u):
        def do(which):
            for i in range(KINDS):
                wait(s5_copy(u, i, which))
                start(*s6_copies(u, i, which))
        on_matrix(u, do)

    def stage7(u):
        def do(which):
            for i in range(KINDS):
                wait(*s6_copies(u, i, which))
                start(s7_copy(u, i, which))
        on_matrix(u, do)

    def stage8(u):
        def do(which):
            for i in range(KINDS):
                wait(s7_copy(u, i, which))
        on_matrix(u, do)

    stages = (stage0, stage1, stage2, stage3, stage4, stage5, stage6, stage7, stage8)
    parts, first = 2 * SPLIT, 3 * SPLIT

    last = layers - 1
    in_a = n // rows_d

    def keep():
        def some(o, _):
            x, y = o // SIDE, lax.rem(o, SIDE)
            to = pl.ds(pl.multiple_of(o * rows_g, 8), rows_g)
            for k, (w, wide) in enumerate(((og_h, wgu), (ou_h, both))):
                half = pl.ds(pl.multiple_of(k * d + o * rows_g, 8), rows_g)
                for c in range(2):
                    at = wide.at[c, to] if k == 0 else wide.at[pl.ds(pl.multiple_of(c * d + o * rows_g, 8), rows_g)]
                    start(load(w.at[last, x, y, :, pl.ds(c * 2 * f, 2 * f)], at, lf.at[2 * k + c]))
                start(load(w.at[last, x, y, :, pl.ds(4 * f, f)], hid.at[half], lf.at[4 + k]))
                start(load(w.at[0, x, y, :, pl.ds(0, d)], dy.at[half], lf.at[6 + k]))

            @pl.when(o < in_a)
            def _():
                start(load(od_h.at[last, x, y], a.at[pl.ds(pl.multiple_of(o * rows_d, 8), rows_d)], lf.at[8]))

            @pl.when(o >= in_a)
            def _():
                start(load(od_h.at[last, x, y], h.at[pl.ds(pl.multiple_of((o - in_a) * rows_d, 8), rows_d)], lf.at[9]))
            return 0

        lax.fori_loop(0, SIDE * SIDE, some, 0)

    def kept():
        half = pl.ds(0, d)
        for c in range(2):
            wait(load(both_h.at[0, half], wgu.at[c], lf.at[c]), load(both_h.at[0, half], both.at[pl.ds(c * d, d)], lf.at[2 + c]))
        for k in range(2):
            wait(load(both_h.at[0, half, pl.ds(0, f)], hid.at[pl.ds(k * d, d)], lf.at[4 + k]),
                 load(dy_h.at[half], dy.at[pl.ds(k * d, d)], lf.at[6 + k]))
        for k, (blocks, to) in enumerate(((in_a, a), (SIDE * SIDE - in_a, h))):
            rows = pl.ds(0, blocks * rows_d)
            wait(load(dy_h.at[rows], to.at[rows], lf.at[8 + k]))

    keep_at = max(first + parts * (per_layer + 3) + WHEN[-1] + 1, parts * (per_layer + 2 * BLOCKS))
    assert d <= 2 * f

    def tick(t, _):
        for when, stage in zip(WHEN, stages, strict=True):
            since = t - first - when + parts * WHEN[-1]
            u = since // parts - WHEN[-1]
            pl.when((u >= 0) & (u < units) & (lax.rem(since, parts) == 0))(functools.partial(stage, u))
        pl.when(t == keep_at)(keep)

        layer = layers - 1 - t // (parts * per_layer)
        k = lax.rem(t, parts * per_layer)
        b, piece, c = k // (2 * parts), lax.rem(k, 2 * parts), k - 2 * parts * BLOCKS
        busy, blocks, start_u = t < parts * units, k < 2 * parts * BLOCKS, (layers - 1 - layer) * per_layer + 2 * b
        pl.when(busy & blocks & (piece < 2 * SPLIT))(lambda: hidden_units(layer, b, piece))
        pl.when(busy & blocks & (piece // SPLIT == 2))(lambda: gradient_columns(start_u, piece - 2 * SPLIT))
        pl.when(busy & blocks & (piece // SPLIT == 3))(lambda: gradient_rows(layer, b, piece - 3 * SPLIT))
        pl.when(busy & ~blocks & (layer > 0))(lambda: states_back(c // parts, lax.rem(c, parts)))
        return 0

    first_units(0)
    start(load_dy)
    lax.fori_loop(1, BLOCKS - 1, lambda b, _: (first_units(b), 0)[1], 0)
    first_units(BLOCKS - 1)
    pl.semaphore_wait(barrier, 4)
    lax.fori_loop(0, first + parts * (units - 1) + WHEN[-1] + 1, tick, 0)
    kept()


def results_kernel(*refs, hidden, count):
    (og, ou, od), moments, kept = refs[:3], refs[3:9], refs[9:15]
    (rg, ru, rd), moved = refs[15:18], refs[18:24]
    bg, bu, bd, bufs, sems = refs[24], refs[25], refs[26], refs[27:33], refs[33]
    a, h, dy, wgu, hid, both = kept
    n, d = a.shape
    f, last = hid.shape[1], rg.shape[0] - 1
    copies = []

    def copy(src, dst):
        copies.append(pltpu.make_async_copy(src, dst, sems.at[len(copies)]))
        return copies[-1]

    through = []
    step = d // 4
    for w, buf, out in ((og, bg, rg), (ou, bu, ru)):
        for r in range(0, d, step):
            at = (pl.ds(r, step), pl.ds(d, hidden - d))
            through.append((copy(w.at[0, *at], buf.at[pl.ds(r, step)]), copy(buf.at[pl.ds(r, step)], out.at[0, *at])))
    step = hidden // 4
    for r in range(0, hidden, step):
        at = pl.ds(r, step)
        through.append((copy(od.at[0, at], bd.at[at]), copy(bd.at[at], rd.at[0, at])))
    for src, buf, out in zip(moments, bufs, moved, strict=True):
        for layer in range(last + 1):
            through.append((copy(src.at[layer], buf.at[layer]), copy(buf.at[layer], out.at[layer])))
    block = hidden // (SIDE * SIDE)
    rows = n // block * block
    straight = [copy(a.at[pl.ds(0, rows)], rd.at[last, pl.ds(0, rows)]), copy(h.at[pl.ds(0, hidden - rows)], rd.at[last, pl.ds(rows, hidden - rows)])]
    for k, out in enumerate((rg, ru)):
        for c in range(2):
            src = both.at[pl.ds(c * d, d)] if k else wgu.at[c]
            straight.append(copy(src, out.at[last, :, pl.ds(c * 2 * f, 2 * f)]))
        straight.append(copy(hid.at[pl.ds(k * d, d)], out.at[last, :, pl.ds(4 * f, f)]))
        straight.append(copy(dy.at[pl.ds(k * d, d)], out.at[0, :, pl.ds(0, d)]))
    assert len(copies) == count
    for i, _ in through:
        i.start()
    for c in straight:
        c.start()
    for i, o in through:
        i.wait()
        o.start()
    for c in (*straight, *(o for _, o in through)):
        c.wait()


def results(arrays, kept):
    (layers, d, hidden), moments = arrays[0].shape, arrays[3:]
    count = 2 * (4 + 4 + 4 + len(moments) * layers) + 10
    vmem = [pltpu.VMEM(s, t) for s, t in (((d, hidden - d), BF), ((d, hidden - d), BF), ((hidden, d), BF), *((m.shape, F32) for m in moments))]
    return pl.pallas_call(
        functools.partial(results_kernel, hidden=hidden, count=count),
        out_shape=[jax.ShapeDtypeStruct(a.shape, a.dtype) for a in arrays],
        in_specs=[pl.BlockSpec(memory_space=pltpu.HBM)] * len(arrays) + [pl.BlockSpec(memory_space=pltpu.VMEM)] * len(kept),
        out_specs=[pl.BlockSpec(memory_space=pltpu.HBM)] * len(arrays),
        scratch_shapes=vmem + [pltpu.SemaphoreType.DMA((count,))],
        compiler_params=pltpu.CompilerParams(vmem_limit_bytes=VLIM),
        name="results",
    )(*(pltpu.with_memory_space_constraint(a, pltpu.HBM) for a in arrays), *(pltpu.with_memory_space_constraint(a, pltpu.VMEM) for a in kept))


def train_step(layers, x, dy, ws, ms, vs):
    n, d = dy.shape
    f = ws[0].shape[2] // BLOCKS
    owners = SIDE * SIDE
    rows_g, rows_d = d // owners, f * BLOCKS // owners
    units = layers * 3 * BLOCKS
    ring = 4
    flat = rows_g * f // KINDS // LANES
    blocks = (SLOTS, KINDS, SIDE, flat, LANES)
    block = (SLOTS, KINDS, flat, LANES)
    gate, down = (2, rows_g, f), (2, rows_d // BLOCKS, d)
    vmem, dma = pltpu.VMEM, pltpu.SemaphoreType.DMA
    sd = jax.ShapeDtypeStruct
    outs = pl.pallas_call(
        functools.partial(step_kernel, layers=layers, units=units, ring=ring),
        out_shape=[sd((layers, SIDE, SIDE, rows_g, f * BLOCKS), BF)] * 2
        + [sd((layers, SIDE, SIDE, rows_d, d), BF)]
        + [sd(m.shape, F32) for m in ms] + [sd(v.shape, F32) for v in vs]
        + [sd((BLOCKS, n, 2 * f), BF)]
        + [vmem((n, d), BF)] * 3 + [vmem((2, d, 2 * f), BF), vmem((n, f), BF), vmem((n, 2 * f), BF)],
        in_specs=[ANY] * 11,
        out_specs=[ANY] * 10 + [pl.BlockSpec(memory_space=pltpu.VMEM)] * 6,
        scratch_shapes=[
            vmem((2, f, d), BF), vmem((n, d), F32),
            vmem((ring, KINDS, SIDE, SIDE, flat, LANES), BF), vmem((BLOCKS + 1, KINDS, SIDE, SIDE, flat, LANES), BF),
            vmem(blocks, BF), vmem(blocks, BF), vmem(blocks, BF), vmem((SLOTS, KINDS, 2, flat, LANES), F32),
            vmem(block, BF), vmem(block, BF), vmem(block, BF),
            vmem(gate, BF), vmem(gate, F32), vmem(gate, F32), vmem(gate, BF), vmem(gate, F32), vmem(gate, F32),
            vmem(down, BF), vmem(down, F32), vmem(down, F32), vmem(down, BF), vmem(down, F32), vmem(down, F32),
            dma((SLOTS, KINDS, 12)), dma((SLOTS, KINDS, 12)),
            dma((2, 3)), dma((n // 256,)), dma((2,)), dma, dma((2, 3)), dma((2, 3)), dma((10,)),
        ],
        compiler_params=pltpu.CompilerParams(collective_id=0, has_side_effects=True, vmem_limit_bytes=VLIM),
        name="train_step",
    )(x, dy, *ws, *ms, *vs)
    return outs[:9], outs[10:]


def solution(mesh):
    assert mesh.shape["dp"] == SIDE * SIDE

    def body(x, dy, *arrays):
        ws, ms, vs = (arrays[i : i + 3] for i in (0, 3, 6))
        x, dy = x[0], dy[0]
        layers = ws[0].shape[0]
        outs, kept = train_step(layers, x, dy, ws, ms, vs)
        return tuple(results([o.reshape(w.shape) for o, w in zip(outs[:3], ws, strict=True)] + list(outs[3:]), kept))

    whole, rows = P(None, None, None), P(None, "dp", None)
    return jax.shard_map(
        body,
        mesh=mesh,
        in_specs=(P(("rep", "dp")),) * 2 + (whole,) * 3 + (rows,) * 6,
        out_specs=(P("rep"),) * 3 + (P("rep", "dp"),) * 6,
        check_vma=False,
    )
```

```python
import functools

import jax
import jax.numpy as jnp
from jax import lax
from jax.experimental import pallas as pl
from jax.experimental.pallas import tpu as pltpu
from jax.sharding import PartitionSpec as P

BF, F32 = jnp.bfloat16, jnp.float32
MESH = pl.DeviceIdType.MESH
SIDE = 4
KINDS = 4
BLOCKS = 5
LANES = 128
WHEN = (0, 1, 2, 3, 4, 5, 7, 8, 9)
UNROLL = 4
VLIM = 38 * 2**20
SLOTS = 4
ANY = pl.BlockSpec(memory_space=pl.ANY)


def dot(a, b, da, db):
    return lax.dot_general(a, b, (((da,), (db,)), ((), ())), preferred_element_type=F32)


def normed(wide):
    return (wide * lax.rsqrt(jnp.mean(wide * wide, -1, keepdims=True) + 1e-6)).astype(BF)


def step_kernel(x_h, dy_h, wg_h, wu_h, wd_h, mg_h, mu_h, md_h, vg_h, vu_h, vd_h,
                og_h, ou_h, od_h, omg_h, omu_h, omd_h, ovg_h, ovu_h, ovd_h, both_h, a, h, dy, wgu, hid, both,
                wd, acc, dwg, dwd,
                r1, r2, r3, t3, q1, q2, q3,
                cw, cm, cv, nw, nm, nv, ew, em, ev, fw, fm, fv,
                ss, rs, lw, la, lb, ls, lp, lo, lf, *, layers, units, ring):
    n, d = a.shape
    f = wd.shape[1]
    rows_g = d // (SIDE * SIDE)
    rows_d = f * BLOCKS // (SIDE * SIDE)
    sub_g, sub_d = rows_g // KINDS, rows_d // BLOCKS
    per_layer = units // layers
    me = lax.axis_index("dp")
    mx, my = me // SIDE, me % SIDE
    wrap = lambda v: lax.rem(v + 2 * SIDE, SIDE)
    dev = lambda x, y: {"dp": wrap(x) * SIDE + wrap(y)}

    barrier = pltpu.get_barrier_semaphore()
    for x, y in ((mx + 1, my), (mx - 1, my), (mx, my + 1), (mx, my - 1)):
        pl.semaphore_signal(barrier, inc=1, device_id=dev(x, y), device_id_type=MESH)

    load = lambda src, dst, sem: lambda: pltpu.make_async_copy(src, dst, sem)

    def start(*copies):
        for c in copies:
            c().start()

    def wait(*copies):
        for c in copies:
            c().wait()

    def weights(w):
        z, b, turn = lax.rem(w, 2), lax.rem(w, BLOCKS), w // BLOCKS
        layer = jnp.where((turn == 0) | (turn == 3), 0, layers - 1)
        cols = pl.ds(pl.multiple_of(b * f, LANES), f)
        rows = pl.ds(pl.multiple_of(b * f, 8), f)
        return (load(wg_h.at[layer, :, cols], wgu.at[z, :, pl.ds(0, f)], lw.at[z, 0]),
                load(wu_h.at[layer, :, cols], wgu.at[z, :, pl.ds(f, f)], lw.at[z, 1]),
                load(wd_h.at[layer, rows, :], wd.at[z], lw.at[z, 2]))

    def next_weights(w):
        wait(*weights(w))
        pl.when(w < 4 * BLOCKS - 1)(lambda: start(*weights(w + 1)))

    saved = lambda b: load(both, both_h.at[b], ls)
    back = lambda b: load(both_h.at[b], both, lb.at[0])
    TILE, NORM = 256, 64
    load_x = [load(x_h.at[pl.ds(t * TILE, TILE), :], h.at[pl.ds(t * TILE, TILE), :], la.at[t]) for t in range(n // TILE)]
    load_dy = load(dy_h, dy, lb.at[1])
    x_to_a = load(x_h, a, lb.at[1])
    start(load_x[0], *weights(0), *load_x[1:])

    def tokens(t, size=TILE):
        return pl.ds(pl.multiple_of(t * size, size), size)

    def loop(count, do, unroll):
        def some(t, _):
            for k in range(unroll):
                do(t * unroll + k)
            return 0

        lax.fori_loop(0, count // unroll, some, 0)

    def every_token(do):
        loop(n // NORM, lambda t: do(tokens(t, NORM)), 1)

    def norm_states(at):
        a[at, :] = normed(h[at, :].astype(F32))

    def first_units(b):
        z = lax.rem(b, 2)
        at_start, at_end = isinstance(b, int) and b == 0, isinstance(b, int) and b == BLOCKS - 1
        next_weights(b)

        def do(t):
            at = tokens(t)
            if at_start:
                pltpu.make_async_copy(x_h.at[at, :], h.at[at, :], la.at[t]).wait()
                norm_states(at)
            gu = dot(a[at, :], wgu[z], 1, 0)
            gate, up = gu[:, :f], gu[:, f:]
            hidden = (gate * jax.nn.sigmoid(gate) * up).astype(BF)
            more = dot(hidden, wd[z], 1, 0)
            if at_end:
                new = h[at, :] + (acc[at, :] + more).astype(BF)
                h[at, :] = new
                a[at, :] = normed(new.astype(F32))
            else:
                acc[at, :] = more if at_start else acc[at, :] + more

        loop(n // TILE, do, UNROLL)

    def clear(at):
        acc[at, :] = jnp.zeros((NORM, d), F32)

    def hidden_units(layer, b, piece):
        w = jnp.where(layer > 0, BLOCKS, 3 * BLOCKS) + b
        z = lax.rem(w, 2)

        @pl.when(piece == 0)
        def _():
            next_weights(w)

            @pl.when((b == 0) & (layer > 0))
            def _():
                wait(load_dy)

        def part(t):
            at = tokens(piece * (n // TILE // 2) + t)
            gu = dot(a[at, :], wgu[z], 1, 0)
            gate, up = gu[:, :f], gu[:, f:]
            back = dot(dy[at, :], wd[z], 1, 1).astype(BF).astype(F32)
            s = jax.nn.sigmoid(gate)
            silu = gate * s
            hid[at, :] = (silu * up).astype(BF)
            both[at, f:] = (back * silu).astype(BF)
            both[at, :f] = (back * up * (s + silu * (1 - s))).astype(BF)

        loop(n // TILE // 2, part, UNROLL)
        pl.when((piece == 1) & (layer > 0))(lambda: start(saved(b)))

    def gradient_columns(u, low, high):
        quarter = d // SIDE

        def part(r):
            r = low + r
            cols = pl.ds(pl.multiple_of(r * quarter, LANES), quarter)
            g = dot(a[:, cols], both[...], 0, 0).astype(BF)
            g = g.reshape(SIDE, KINDS, sub_g, 2 * f)
            for which in range(2):
                slot = lax.rem(u + which, ring)
                for i in range(KINDS):
                    for c in range(f // LANES):
                        at = which * f + c * LANES
                        dwg[slot, i, r, :, c * sub_g : (c + 1) * sub_g, :] = g[:, i, :, at : at + LANES]

        loop(high - low, part, high - low)

    def gradient_rows(layer, b):
        cols_k = d // KINDS

        def part(i):
            cols = pl.ds(pl.multiple_of(i * cols_k, LANES), cols_k)
            g = dot(hid[...], dy[:, cols], 0, 0).astype(BF)
            for k in range(f // sub_d):
                unit = b * (f // sub_d) + k
                owner, j = unit // BLOCKS, unit % BLOCKS
                slot = lax.rem((layers - 1 - layer) * BLOCKS + j, dwd.shape[0])
                for c in range(cols_k // LANES):
                    dwd[slot, i, owner // SIDE, owner % SIDE, c * sub_d : (c + 1) * sub_d, :] = (
                        g[k * sub_d : (k + 1) * sub_d, c * LANES : (c + 1) * LANES])

        loop(KINDS, part, UNROLL)

        @pl.when(layer > 0)
        def _():
            wait(saved(b))
            pl.when(b == BLOCKS - 1)(lambda: start(back(0), x_to_a))

    def states_back(q, piece):
        w = 2 * BLOCKS + q
        z = lax.rem(w, 2)

        @pl.when(piece == 0)
        def _():
            pl.when(q == 0)(lambda: every_token(clear))
            next_weights(w)
            wait(back(q))

        def part(t):
            at = tokens(piece * (n // TILE // 2) + t)
            acc[at, :] = acc[at, :] + dot(both[at, :], wgu[z], 1, 1)

        loop(n // TILE // 2, part, UNROLL)
        pl.when((piece == 1) & (q < BLOCKS - 1))(lambda: start(back(q + 1)))
        half = n // NORM // 2

        @pl.when((q == 1) | (q == 2))
        def _():
            pl.when((q == 1) & (piece == 0))(lambda: wait(x_to_a))

            def do(t):
                at = tokens((2 * (q - 1) + piece) * (half // 2) + t, NORM)
                a[at, :] = normed(a[at, :].astype(F32))

            loop(half // 2, do, 1)

        @pl.when(q == BLOCKS - 1)
        def _():
            def do(t):
                at = tokens(piece * half + t, NORM)
                wide = h[at, :].astype(F32)
                scale = lax.rsqrt(jnp.mean(wide * wide, -1, keepdims=True) + 1e-6)
                by = acc[at, :].astype(BF).astype(F32)
                along = jnp.mean(by * wide, -1, keepdims=True)
                more = by * scale - wide * (scale * scale * scale * along)
                dy[at, :] = (dy[at, :].astype(F32) + more.astype(BF).astype(F32)).astype(BF)

            loop(half, do, 1)

    def place(u):
        k = lax.rem(u, per_layer)
        return layers - 1 - u // per_layer, jnp.where(k >= 2 * BLOCKS, k - 2 * BLOCKS, k // 2)

    def steps(i):
        s = 1 - 2 * (i % 2)
        xs, ys = (dev(mx + s, my), dev(mx - s, my)), (dev(mx, my + s), dev(mx, my - s))
        return (*xs, *ys, mx, my, s) if i < 2 else (*ys, *xs, my, mx, s)

    def rcopy(src, dst, u, i, k, to):
        n_ = lax.rem(u, SLOTS)
        return lambda: pltpu.make_async_remote_copy(
            src_ref=src, dst_ref=dst, send_sem=ss.at[n_, i, k], recv_sem=rs.at[n_, i, k], device_id=to, device_id_type=MESH)

    def own(u, i, p, which):
        w = dwd.at[lax.rem(u // per_layer * BLOCKS + place(u)[1], dwd.shape[0]), i] if which else dwg.at[lax.rem(u, ring), i]
        return w.at[p] if i < 2 else w.at[:, p]

    def on_own(u, do):
        k = lax.rem(u, per_layer)
        pl.when(k < 2 * BLOCKS)(lambda: do(0))
        pl.when(k >= 2 * BLOCKS)(lambda: do(1))

    def s0_copies(u, i, which):
        ahead, behind, _, _, pf, _, s = steps(i)
        n_ = lax.rem(u, SLOTS)
        return (rcopy(own(u, i, wrap(pf + 2), which), r1.at[n_, i], u, i, 0, ahead),
                rcopy(own(u, i, wrap(pf - s), which), r2.at[n_, i], u, i, 1, behind))

    def s1_copy(u, i):
        n_ = lax.rem(u, SLOTS)
        return rcopy(r1.at[n_, i], r3.at[n_, i], u, i, 2, steps(i)[0])

    def s2_copies(u, i):
        _, _, ahead, behind, _, ps, s = steps(i)
        n_ = lax.rem(u, SLOTS)
        return (rcopy(r3.at[n_, i, wrap(ps + 2)], q1.at[n_, i], u, i, 3, ahead),
                rcopy(r3.at[n_, i, wrap(ps - s)], q2.at[n_, i], u, i, 4, behind))

    def s3_copy(u, i):
        n_ = lax.rem(u, SLOTS)
        return rcopy(q1.at[n_, i], q3.at[n_, i], u, i, 5, steps(i)[2])

    def state_copies(u, which, out):
        layer, j = place(u)
        z = lax.rem(u, 2)
        cols = pl.ds(pl.multiple_of(j * f, LANES), f)
        rows = pl.ds(pl.multiple_of(me * rows_d + j * sub_d, 8), sub_d)
        mine = pl.ds(pl.multiple_of(j * sub_d, 8), sub_d)
        first = pl.ds(pl.multiple_of(me * rows_g, 8), rows_g)
        if which < 2:
            if out:
                w, m, v = ((og_h, omg_h, ovg_h), (ou_h, omu_h, ovu_h))[which]
                return (load(nw.at[z], w.at[layer, mx, my, :, cols], lo.at[z, 0]), load(nm.at[z], m.at[layer, :, cols], lo.at[z, 1]),
                        load(nv.at[z], v.at[layer, :, cols], lo.at[z, 2]))
            w, m, v = ((wg_h, mg_h, vg_h), (wu_h, mu_h, vu_h))[which]
            return (load(w.at[layer, first, cols], cw.at[z], lp.at[z, 0]), load(m.at[layer, :, cols], cm.at[z], lp.at[z, 1]),
                    load(v.at[layer, :, cols], cv.at[z], lp.at[z, 2]))
        if out:
            return (load(fw.at[z], od_h.at[layer, mx, my, mine, :], lo.at[z, 0]), load(fm.at[z], omd_h.at[layer, mine, :], lo.at[z, 1]),
                    load(fv.at[z], ovd_h.at[layer, mine, :], lo.at[z, 2]))
        return (load(wd_h.at[layer, rows, :], ew.at[z], lp.at[z, 0]), load(md_h.at[layer, mine, :], em.at[z], lp.at[z, 1]),
                load(vd_h.at[layer, mine, :], ev.at[z], lp.at[z, 2]))

    def on_matrix(u, do):
        k = lax.rem(u, per_layer)
        down = k >= 2 * BLOCKS
        for which, test in enumerate((~down & (lax.rem(k, 2) == 0), ~down & (lax.rem(k, 2) == 1), down)):
            pl.when(test)(functools.partial(do, which))

    def out_at(u, i, which):
        layer, j = place(u)
        if which < 2:
            cols = pl.ds(pl.multiple_of(j * f, LANES), f)
            return lambda x, y: (og_h, ou_h)[which].at[layer, x, y, pl.ds(i * sub_g, sub_g), cols]
        rows = pl.ds(pl.multiple_of(j * sub_d, 8), sub_d)
        wide = d // KINDS
        return lambda x, y: od_h.at[layer, x, y, rows, pl.ds(i * wide, wide)]

    def s4_copies(u, i, which):
        _, _, ahead, behind, _, _, _ = steps(i)
        z = lax.rem(u, 2)
        wide = d // KINDS
        dst = out_at(u, i, which)(mx, my)
        src = nw.at[z, pl.ds(i * sub_g, sub_g), :] if which < 2 else fw.at[z, :, pl.ds(i * wide, wide)]
        return (rcopy(src, dst, u, i, 6, ahead), rcopy(src, dst, u, i, 7, behind))

    def s5_copy(u, i, which):
        _, _, ahead, _, pf, ps, s = steps(i)
        at = out_at(u, i, which)
        src = at(pf, wrap(ps - s)) if i < 2 else at(wrap(ps - s), pf)
        return rcopy(src, src, u, i, 8, ahead)

    every = pl.ds(0, SIDE)

    def s6_copies(u, i, which):
        ahead, behind, _, _, pf, _, _ = steps(i)
        at = out_at(u, i, which)
        src = at(pf, every) if i < 2 else at(every, pf)
        return (rcopy(src, src, u, i, 9, ahead), rcopy(src, src, u, i, 10, behind))

    def s7_copy(u, i, which):
        ahead, _, _, _, pf, _, s = steps(i)
        at = out_at(u, i, which)
        p = wrap(pf - s)
        src = at(p, every) if i < 2 else at(every, p)
        return rcopy(src, src, u, i, 11, ahead)

    def stage0(u):
        def do(which):
            for i in range(KINDS):
                start(*s0_copies(u, i, which))
        on_own(u, do)

    def stage1(u):
        n_ = lax.rem(u, SLOTS)

        def do(which):
            for i in range(KINDS):
                _, _, _, _, pf, _, s = steps(i)
                wait(s0_copies(u, i, which)[0])
                mine = own(u, i, wrap(pf + s), which)
                r1[n_, i] = (r1[n_, i].astype(F32) + mine[...].astype(F32)).astype(BF)
                start(s1_copy(u, i))
        on_own(u, do)

    def stage2(u):
        n_ = lax.rem(u, SLOTS)

        def do(which):
            for i in range(KINDS):
                _, _, _, _, pf, ps, s = steps(i)
                wait(s0_copies(u, i, which)[1], s1_copy(u, i))
                mine = own(u, i, pf, which)
                for k in (2, -s, s, 0):
                    p = wrap(ps + k)
                    total = r2[n_, i, p].astype(F32) + r3[n_, i, p].astype(F32) + mine[p].astype(F32)
                    if k in (2, -s):
                        r3[n_, i, p] = total.astype(BF)
                    else:
                        t3[n_, i, 0 if k else 1] = total
                start(*s2_copies(u, i))
        on_own(u, do)

    def stage3(u):
        n_ = lax.rem(u, SLOTS)
        on_matrix(u, lambda which: start(*state_copies(u, which, False)))
        for i in range(KINDS):
            wait(s2_copies(u, i)[0])
            q1[n_, i] = (q1[n_, i].astype(F32) + t3[n_, i, 0]).astype(BF)
            start(s3_copy(u, i))

    def stage4(u):
        n_, z = lax.rem(u, SLOTS), lax.rem(u, 2)

        def update(g, w, m, v):
            g = g.astype(BF).astype(F32)
            m = 0.9 * m + 0.1 * g
            v = 0.95 * v + 0.05 * g * g
            w = w.astype(F32)
            return (w - 0.02 * (m * lax.rsqrt(v + 1e-8) + 0.1 * w)).astype(BF), m, v

        for i in range(KINDS):
            wait(s2_copies(u, i)[1], s3_copy(u, i))

        def do(which):
            wait(*state_copies(u, which, False))
            wide, sub = d // KINDS, sub_g if which < 2 else sub_d
            for i in range(KINDS):
                for c in range(r1.shape[3] // sub):
                    part = pl.ds(c * sub, sub)
                    g = q2[n_, i, part, :].astype(F32) + q3[n_, i, part, :].astype(F32) + t3[n_, i, 1, part, :]
                    if which < 2:
                        at = (z, pl.ds(i * sub, sub), pl.ds(c * LANES, LANES))
                        nw[at], nm[at], nv[at] = update(g, cw[at], cm[at], cv[at])
                    else:
                        at = (z, slice(None), pl.ds(i * wide + c * LANES, LANES))
                        fw[at], fm[at], fv[at] = update(g, ew[at], em[at], ev[at])
                start(*s4_copies(u, i, which))
            start(*state_copies(u, which, True))
        on_matrix(u, do)

    def stage5(u):
        def do(which):
            wait(*state_copies(u, which, True))
            for i in range(KINDS):
                wait(*s4_copies(u, i, which))
                start(s5_copy(u, i, which))
        on_matrix(u, do)

    def stage6(u):
        def do(which):
            for i in range(KINDS):
                wait(s5_copy(u, i, which))
                start(*s6_copies(u, i, which))
        on_matrix(u, do)

    def stage7(u):
        def do(which):
            for i in range(KINDS):
                wait(*s6_copies(u, i, which))
                start(s7_copy(u, i, which))
        on_matrix(u, do)

    def stage8(u):
        def do(which):
            for i in range(KINDS):
                wait(s7_copy(u, i, which))
        on_matrix(u, do)

    stages = (stage0, stage1, stage2, stage3, stage4, stage5, stage6, stage7, stage8)
    parts, first = 2, 4

    last = layers - 1
    in_a = n // rows_d

    def keep():
        def some(o, _):
            x, y = o // SIDE, lax.rem(o, SIDE)
            to = pl.ds(pl.multiple_of(o * rows_g, 8), rows_g)
            for k, (w, wide) in enumerate(((og_h, wgu), (ou_h, both))):
                half = pl.ds(pl.multiple_of(k * d + o * rows_g, 8), rows_g)
                for c in range(2):
                    at = wide.at[c, to] if k == 0 else wide.at[pl.ds(pl.multiple_of(c * d + o * rows_g, 8), rows_g)]
                    start(load(w.at[last, x, y, :, pl.ds(c * 2 * f, 2 * f)], at, lf.at[2 * k + c]))
                start(load(w.at[last, x, y, :, pl.ds(4 * f, f)], hid.at[half], lf.at[4 + k]))
                start(load(w.at[0, x, y, :, pl.ds(0, d)], dy.at[half], lf.at[6 + k]))

            @pl.when(o < in_a)
            def _():
                start(load(od_h.at[last, x, y], a.at[pl.ds(pl.multiple_of(o * rows_d, 8), rows_d)], lf.at[8]))

            @pl.when(o >= in_a)
            def _():
                start(load(od_h.at[last, x, y], h.at[pl.ds(pl.multiple_of((o - in_a) * rows_d, 8), rows_d)], lf.at[9]))
            return 0

        lax.fori_loop(0, SIDE * SIDE, some, 0)

    def kept():
        half = pl.ds(0, d)
        for c in range(2):
            wait(load(both_h.at[0, half], wgu.at[c], lf.at[c]), load(both_h.at[0, half], both.at[pl.ds(c * d, d)], lf.at[2 + c]))
        for k in range(2):
            wait(load(both_h.at[0, half, pl.ds(0, f)], hid.at[pl.ds(k * d, d)], lf.at[4 + k]),
                 load(dy_h.at[half], dy.at[pl.ds(k * d, d)], lf.at[6 + k]))
        for k, (blocks, to) in enumerate(((in_a, a), (SIDE * SIDE - in_a, h))):
            rows = pl.ds(0, blocks * rows_d)
            wait(load(dy_h.at[rows], to.at[rows], lf.at[8 + k]))

    keep_at = max(first + parts * (per_layer + 3) + WHEN[-1] + 1, parts * (per_layer + 2 * BLOCKS))
    assert d <= 2 * f

    def tick(t, _):
        for when, stage in zip(WHEN, stages, strict=True):
            since = t - first - when + parts * WHEN[-1]
            u = since // parts - WHEN[-1]
            pl.when((u >= 0) & (u < units) & (lax.rem(since, parts) == 0))(functools.partial(stage, u))
        pl.when(t == keep_at)(keep)

        layer = layers - 1 - t // (parts * per_layer)
        k = lax.rem(t, parts * per_layer)
        b, piece, c = k // 4, lax.rem(k, 4), k - 4 * BLOCKS
        busy, blocks, u = t < parts * units, k < 4 * BLOCKS, (layers - 1 - layer) * per_layer + 2 * b
        pl.when(busy & blocks & (piece < 2))(lambda: hidden_units(layer, b, piece))
        pl.when(busy & blocks & (piece == 2))(lambda: gradient_columns(u, 0, SIDE - 1))

        @pl.when(busy & blocks & (piece == 3))
        def _():
            gradient_columns(u, SIDE - 1, SIDE)
            gradient_rows(layer, b)

        pl.when(busy & ~blocks & (layer > 0))(lambda: states_back(c // 2, lax.rem(c, 2)))
        return 0

    first_units(0)
    start(load_dy)
    lax.fori_loop(1, BLOCKS - 1, lambda b, _: (first_units(b), 0)[1], 0)
    first_units(BLOCKS - 1)
    pl.semaphore_wait(barrier, 4)
    lax.fori_loop(0, first + parts * (units - 1) + WHEN[-1] + 1, tick, 0)
    kept()


def results_kernel(*refs, hidden, count):
    (og, ou, od), moments, kept = refs[:3], refs[3:9], refs[9:15]
    (rg, ru, rd), moved = refs[15:18], refs[18:24]
    bg, bu, bd, bufs, sems = refs[24], refs[25], refs[26], refs[27:33], refs[33]
    a, h, dy, wgu, hid, both = kept
    n, d = a.shape
    f, last = hid.shape[1], rg.shape[0] - 1
    copies = []

    def copy(src, dst):
        copies.append(pltpu.make_async_copy(src, dst, sems.at[len(copies)]))
        return copies[-1]

    through = []
    step = d // 4
    for w, buf, out in ((og, bg, rg), (ou, bu, ru)):
        for r in range(0, d, step):
            at = (pl.ds(r, step), pl.ds(d, hidden - d))
            through.append((copy(w.at[0, *at], buf.at[pl.ds(r, step)]), copy(buf.at[pl.ds(r, step)], out.at[0, *at])))
    step = hidden // 4
    for r in range(0, hidden, step):
        at = pl.ds(r, step)
        through.append((copy(od.at[0, at], bd.at[at]), copy(bd.at[at], rd.at[0, at])))
    for src, buf, out in zip(moments, bufs, moved, strict=True):
        for layer in range(last + 1):
            through.append((copy(src.at[layer], buf.at[layer]), copy(buf.at[layer], out.at[layer])))
    block = hidden // (SIDE * SIDE)
    rows = n // block * block
    straight = [copy(a.at[pl.ds(0, rows)], rd.at[last, pl.ds(0, rows)]), copy(h.at[pl.ds(0, hidden - rows)], rd.at[last, pl.ds(rows, hidden - rows)])]
    for k, out in enumerate((rg, ru)):
        for c in range(2):
            src = both.at[pl.ds(c * d, d)] if k else wgu.at[c]
            straight.append(copy(src, out.at[last, :, pl.ds(c * 2 * f, 2 * f)]))
        straight.append(copy(hid.at[pl.ds(k * d, d)], out.at[last, :, pl.ds(4 * f, f)]))
        straight.append(copy(dy.at[pl.ds(k * d, d)], out.at[0, :, pl.ds(0, d)]))
    assert len(copies) == count
    for i, _ in through:
        i.start()
    for c in straight:
        c.start()
    for i, o in through:
        i.wait()
        o.start()
    for c in (*straight, *(o for _, o in through)):
        c.wait()


def results(arrays, kept):
    (layers, d, hidden), moments = arrays[0].shape, arrays[3:]
    count = 2 * (4 + 4 + 4 + len(moments) * layers) + 10
    vmem = [pltpu.VMEM(s, t) for s, t in (((d, hidden - d), BF), ((d, hidden - d), BF), ((hidden, d), BF), *((m.shape, F32) for m in moments))]
    return pl.pallas_call(
        functools.partial(results_kernel, hidden=hidden, count=count),
        out_shape=[jax.ShapeDtypeStruct(a.shape, a.dtype) for a in arrays],
        in_specs=[pl.BlockSpec(memory_space=pltpu.HBM)] * len(arrays) + [pl.BlockSpec(memory_space=pltpu.VMEM)] * len(kept),
        out_specs=[pl.BlockSpec(memory_space=pltpu.HBM)] * len(arrays),
        scratch_shapes=vmem + [pltpu.SemaphoreType.DMA((count,))],
        compiler_params=pltpu.CompilerParams(vmem_limit_bytes=VLIM),
        name="results",
    )(*(pltpu.with_memory_space_constraint(a, pltpu.HBM) for a in arrays), *(pltpu.with_memory_space_constraint(a, pltpu.VMEM) for a in kept))


def train_step(layers, x, dy, ws, ms, vs):
    n, d = dy.shape
    f = ws[0].shape[2] // BLOCKS
    owners = SIDE * SIDE
    rows_g, rows_d = d // owners, f * BLOCKS // owners
    units = layers * 3 * BLOCKS
    ring = 4
    flat = rows_g * f // KINDS // LANES
    blocks = (SLOTS, KINDS, SIDE, flat, LANES)
    block = (SLOTS, KINDS, flat, LANES)
    gate, down = (2, rows_g, f), (2, rows_d // BLOCKS, d)
    vmem, dma = pltpu.VMEM, pltpu.SemaphoreType.DMA
    sd = jax.ShapeDtypeStruct
    outs = pl.pallas_call(
        functools.partial(step_kernel, layers=layers, units=units, ring=ring),
        out_shape=[sd((layers, SIDE, SIDE, rows_g, f * BLOCKS), BF)] * 2
        + [sd((layers, SIDE, SIDE, rows_d, d), BF)]
        + [sd(m.shape, F32) for m in ms] + [sd(v.shape, F32) for v in vs]
        + [sd((BLOCKS, n, 2 * f), BF)]
        + [vmem((n, d), BF)] * 3 + [vmem((2, d, 2 * f), BF), vmem((n, f), BF), vmem((n, 2 * f), BF)],
        in_specs=[ANY] * 11,
        out_specs=[ANY] * 10 + [pl.BlockSpec(memory_space=pltpu.VMEM)] * 6,
        scratch_shapes=[
            vmem((2, f, d), BF), vmem((n, d), F32),
            vmem((ring, KINDS, SIDE, SIDE, flat, LANES), BF), vmem((BLOCKS + 1, KINDS, SIDE, SIDE, flat, LANES), BF),
            vmem(blocks, BF), vmem(blocks, BF), vmem(blocks, BF), vmem((SLOTS, KINDS, 2, flat, LANES), F32),
            vmem(block, BF), vmem(block, BF), vmem(block, BF),
            vmem(gate, BF), vmem(gate, F32), vmem(gate, F32), vmem(gate, BF), vmem(gate, F32), vmem(gate, F32),
            vmem(down, BF), vmem(down, F32), vmem(down, F32), vmem(down, BF), vmem(down, F32), vmem(down, F32),
            dma((SLOTS, KINDS, 12)), dma((SLOTS, KINDS, 12)),
            dma((2, 3)), dma((n // 256,)), dma((2,)), dma, dma((2, 3)), dma((2, 3)), dma((10,)),
        ],
        compiler_params=pltpu.CompilerParams(collective_id=0, has_side_effects=True, vmem_limit_bytes=VLIM),
        name="train_step",
    )(x, dy, *ws, *ms, *vs)
    return outs[:9], outs[10:]


def solution(mesh):
    assert mesh.shape["dp"] == SIDE * SIDE

    def body(x, dy, *arrays):
        ws, ms, vs = (arrays[i : i + 3] for i in (0, 3, 6))
        x, dy = x[0], dy[0]
        layers = ws[0].shape[0]
        outs, kept = train_step(layers, x, dy, ws, ms, vs)
        return tuple(results([o.reshape(w.shape) for o, w in zip(outs[:3], ws, strict=True)] + list(outs[3:]), kept))

    whole, rows = P(None, None, None), P(None, "dp", None)
    return jax.shard_map(
        body,
        mesh=mesh,
        in_specs=(P(("rep", "dp")),) * 2 + (whole,) * 3 + (rows,) * 6,
        out_specs=(P("rep"),) * 3 + (P("rep", "dp"),) * 6,
        check_vma=False,
    )
```

```python
import functools

import jax
import jax.numpy as jnp
from jax import lax
from jax.experimental import pallas as pl
from jax.experimental.pallas import tpu as pltpu
from jax.sharding import PartitionSpec as P

BF, F32 = jnp.bfloat16, jnp.float32
MESH = pl.DeviceIdType.MESH
SIDE = 4
KINDS = 4
BLOCKS = 5
LANES = 128
WHEN = (0, 1, 2, 3, 4, 5, 7, 8, 9)
UNROLL = 2
VLIM = 38 * 2**20
SLOTS = 4
ANY = pl.BlockSpec(memory_space=pl.ANY)


def dot(a, b, da, db):
    return lax.dot_general(a, b, (((da,), (db,)), ((), ())), preferred_element_type=F32)


def normed(wide):
    return (wide * lax.rsqrt(jnp.mean(wide * wide, -1, keepdims=True) + 1e-6)).astype(BF)


def step_kernel(x_h, dy_h, wg_h, wu_h, wd_h, mg_h, mu_h, md_h, vg_h, vu_h, vd_h,
                og_h, ou_h, od_h, omg_h, omu_h, omd_h, ovg_h, ovu_h, ovd_h, both_h, a, h, dy, wgu, hid, both,
                wd, acc, dwg, dwd,
                r1, r2, r3, t3, q1, q2, q3,
                cw, cm, cv, nw, nm, nv, ew, em, ev, fw, fm, fv,
                ss, rs, lw, la, lb, ls, lp, lo, lf, *, layers, units, ring):
    n, d = a.shape
    f = wd.shape[1]
    rows_g = d // (SIDE * SIDE)
    rows_d = f * BLOCKS // (SIDE * SIDE)
    sub_g, sub_d = rows_g // KINDS, rows_d // BLOCKS
    per_layer = units // layers
    me = lax.axis_index("dp")
    mx, my = me // SIDE, me % SIDE
    wrap = lambda v: lax.rem(v + 2 * SIDE, SIDE)
    dev = lambda x, y: {"dp": wrap(x) * SIDE + wrap(y)}

    barrier = pltpu.get_barrier_semaphore()
    for x, y in ((mx + 1, my), (mx - 1, my), (mx, my + 1), (mx, my - 1)):
        pl.semaphore_signal(barrier, inc=1, device_id=dev(x, y), device_id_type=MESH)

    load = lambda src, dst, sem: lambda: pltpu.make_async_copy(src, dst, sem)

    def start(*copies):
        for c in copies:
            c().start()

    def wait(*copies):
        for c in copies:
            c().wait()

    def weights(w):
        z, b, turn = lax.rem(w, 2), lax.rem(w, BLOCKS), w // BLOCKS
        layer = jnp.where((turn == 0) | (turn == 3), 0, layers - 1)
        cols = pl.ds(pl.multiple_of(b * f, LANES), f)
        rows = pl.ds(pl.multiple_of(b * f, 8), f)
        return (load(wg_h.at[layer, :, cols], wgu.at[z, :, pl.ds(0, f)], lw.at[z, 0]),
                load(wu_h.at[layer, :, cols], wgu.at[z, :, pl.ds(f, f)], lw.at[z, 1]),
                load(wd_h.at[layer, rows, :], wd.at[z], lw.at[z, 2]))

    def next_weights(w):
        wait(*weights(w))
        pl.when(w < 4 * BLOCKS - 1)(lambda: start(*weights(w + 1)))

    saved = lambda b: load(both, both_h.at[b], ls)
    back = lambda b: load(both_h.at[b], both, lb.at[0])
    TILE, NORM = 512, 64
    load_x = [load(x_h.at[pl.ds(t * TILE, TILE), :], h.at[pl.ds(t * TILE, TILE), :], la.at[t]) for t in range(n // TILE)]
    load_dy = load(dy_h, dy, lb.at[1])
    x_to_a = load(x_h, a, lb.at[1])
    start(load_x[0], *weights(0), *load_x[1:])

    def tokens(t, size=TILE):
        return pl.ds(pl.multiple_of(t * size, size), size)

    def loop(count, do, unroll):
        def some(t, _):
            for k in range(unroll):
                do(t * unroll + k)
            return 0

        if count == unroll:
            some(0, 0)
        else:
            lax.fori_loop(0, count // unroll, some, 0)

    def every_token(do):
        loop(n // NORM, lambda t: do(tokens(t, NORM)), 1)

    def norm_states(at):
        a[at, :] = normed(h[at, :].astype(F32))

    def first_units(b):
        z = lax.rem(b, 2)
        at_start, at_end = isinstance(b, int) and b == 0, isinstance(b, int) and b == BLOCKS - 1
        next_weights(b)

        def do(t):
            at = tokens(t)
            if at_start:
                pltpu.make_async_copy(x_h.at[at, :], h.at[at, :], la.at[t]).wait()
                norm_states(at)
            gu = dot(a[at, :], wgu[z], 1, 0)
            gate, up = gu[:, :f], gu[:, f:]
            hidden = (gate * jax.nn.sigmoid(gate) * up).astype(BF)
            more = dot(hidden, wd[z], 1, 0)
            if at_end:
                new = h[at, :] + (acc[at, :] + more).astype(BF)
                h[at, :] = new
                a[at, :] = normed(new.astype(F32))
            else:
                acc[at, :] = more if at_start else acc[at, :] + more

        loop(n // TILE, do, UNROLL)

    def clear(at):
        acc[at, :] = jnp.zeros((NORM, d), F32)

    def hidden_units(layer, b, piece):
        w = jnp.where(layer > 0, BLOCKS, 3 * BLOCKS) + b
        z = lax.rem(w, 2)

        @pl.when(piece == 0)
        def _():
            next_weights(w)

            @pl.when((b == 0) & (layer > 0))
            def _():
                wait(load_dy)

        def part(t):
            at = tokens(piece * (n // TILE // 2) + t)
            gu = dot(a[at, :], wgu[z], 1, 0)
            gate, up = gu[:, :f], gu[:, f:]
            back = dot(dy[at, :], wd[z], 1, 1).astype(BF).astype(F32)
            s = jax.nn.sigmoid(gate)
            silu = gate * s
            hid[at, :] = (silu * up).astype(BF)
            both[at, f:] = (back * silu).astype(BF)
            both[at, :f] = (back * up * (s + silu * (1 - s))).astype(BF)

        loop(n // TILE // 2, part, UNROLL)
        pl.when((piece == 1) & (layer > 0))(lambda: start(saved(b)))

    def gradient_columns(u, low, high):
        quarter = d // SIDE

        def part(r):
            r = low + r
            cols = pl.ds(pl.multiple_of(r * quarter, LANES), quarter)
            g = dot(a[:, cols], both[...], 0, 0).astype(BF)
            g = g.reshape(SIDE, KINDS, sub_g, 2 * f)
            for which in range(2):
                slot = lax.rem(u + which, ring)
                for i in range(KINDS):
                    for c in range(f // LANES):
                        at = which * f + c * LANES
                        dwg[slot, i, r, :, c * sub_g : (c + 1) * sub_g, :] = g[:, i, :, at : at + LANES]

        loop(high - low, part, high - low)

    def gradient_rows(layer, b):
        cols_k = d // KINDS

        def part(i):
            cols = pl.ds(pl.multiple_of(i * cols_k, LANES), cols_k)
            g = dot(hid[...], dy[:, cols], 0, 0).astype(BF)
            for k in range(f // sub_d):
                unit = b * (f // sub_d) + k
                owner, j = unit // BLOCKS, unit % BLOCKS
                slot = lax.rem((layers - 1 - layer) * BLOCKS + j, dwd.shape[0])
                for c in range(cols_k // LANES):
                    dwd[slot, i, owner // SIDE, owner % SIDE, c * sub_d : (c + 1) * sub_d, :] = (
                        g[k * sub_d : (k + 1) * sub_d, c * LANES : (c + 1) * LANES])

        loop(KINDS, part, KINDS)

        @pl.when(layer > 0)
        def _():
            wait(saved(b))
            pl.when(b == BLOCKS - 1)(lambda: start(back(0), x_to_a))

    def states_back(q, piece):
        w = 2 * BLOCKS + q
        z = lax.rem(w, 2)

        @pl.when(piece == 0)
        def _():
            pl.when(q == 0)(lambda: every_token(clear))
            next_weights(w)
            wait(back(q))

        def part(t):
            at = tokens(piece * (n // TILE // 2) + t)
            acc[at, :] = acc[at, :] + dot(both[at, :], wgu[z], 1, 1)

        loop(n // TILE // 2, part, UNROLL)
        pl.when((piece == 1) & (q < BLOCKS - 1))(lambda: start(back(q + 1)))
        half = n // NORM // 2

        @pl.when((q == 1) | (q == 2))
        def _():
            pl.when((q == 1) & (piece == 0))(lambda: wait(x_to_a))

            def do(t):
                at = tokens((2 * (q - 1) + piece) * (half // 2) + t, NORM)
                a[at, :] = normed(a[at, :].astype(F32))

            loop(half // 2, do, 1)

        @pl.when(q == BLOCKS - 1)
        def _():
            def do(t):
                at = tokens(piece * half + t, NORM)
                wide = h[at, :].astype(F32)
                scale = lax.rsqrt(jnp.mean(wide * wide, -1, keepdims=True) + 1e-6)
                by = acc[at, :].astype(BF).astype(F32)
                along = jnp.mean(by * wide, -1, keepdims=True)
                more = by * scale - wide * (scale * scale * scale * along)
                dy[at, :] = (dy[at, :].astype(F32) + more.astype(BF).astype(F32)).astype(BF)

            loop(half, do, 1)

    def place(u):
        k = lax.rem(u, per_layer)
        return layers - 1 - u // per_layer, jnp.where(k >= 2 * BLOCKS, k - 2 * BLOCKS, k // 2)

    def steps(i):
        s = 1 - 2 * (i % 2)
        xs, ys = (dev(mx + s, my), dev(mx - s, my)), (dev(mx, my + s), dev(mx, my - s))
        return (*xs, *ys, mx, my, s) if i < 2 else (*ys, *xs, my, mx, s)

    def rcopy(src, dst, u, i, k, to):
        n_ = lax.rem(u, SLOTS)
        return lambda: pltpu.make_async_remote_copy(
            src_ref=src, dst_ref=dst, send_sem=ss.at[n_, i, k], recv_sem=rs.at[n_, i, k], device_id=to, device_id_type=MESH)

    def own(u, i, p, which):
        w = dwd.at[lax.rem(u // per_layer * BLOCKS + place(u)[1], dwd.shape[0]), i] if which else dwg.at[lax.rem(u, ring), i]
        return w.at[p] if i < 2 else w.at[:, p]

    def on_own(u, do):
        k = lax.rem(u, per_layer)
        pl.when(k < 2 * BLOCKS)(lambda: do(0))
        pl.when(k >= 2 * BLOCKS)(lambda: do(1))

    def s0_copies(u, i, which):
        ahead, behind, _, _, pf, _, s = steps(i)
        n_ = lax.rem(u, SLOTS)
        return (rcopy(own(u, i, wrap(pf + 2), which), r1.at[n_, i], u, i, 0, ahead),
                rcopy(own(u, i, wrap(pf - s), which), r2.at[n_, i], u, i, 1, behind))

    def s1_copy(u, i):
        n_ = lax.rem(u, SLOTS)
        return rcopy(r1.at[n_, i], r3.at[n_, i], u, i, 2, steps(i)[0])

    def s2_copies(u, i):
        _, _, ahead, behind, _, ps, s = steps(i)
        n_ = lax.rem(u, SLOTS)
        return (rcopy(r3.at[n_, i, wrap(ps + 2)], q1.at[n_, i], u, i, 3, ahead),
                rcopy(r3.at[n_, i, wrap(ps - s)], q2.at[n_, i], u, i, 4, behind))

    def s3_copy(u, i):
        n_ = lax.rem(u, SLOTS)
        return rcopy(q1.at[n_, i], q3.at[n_, i], u, i, 5, steps(i)[2])

    def state_copies(u, which, out):
        layer, j = place(u)
        z = lax.rem(u, 2)
        cols = pl.ds(pl.multiple_of(j * f, LANES), f)
        rows = pl.ds(pl.multiple_of(me * rows_d + j * sub_d, 8), sub_d)
        mine = pl.ds(pl.multiple_of(j * sub_d, 8), sub_d)
        first = pl.ds(pl.multiple_of(me * rows_g, 8), rows_g)
        if which < 2:
            if out:
                w, m, v = ((og_h, omg_h, ovg_h), (ou_h, omu_h, ovu_h))[which]
                return (load(nw.at[z], w.at[layer, mx, my, :, cols], lo.at[z, 0]), load(nm.at[z], m.at[layer, :, cols], lo.at[z, 1]),
                        load(nv.at[z], v.at[layer, :, cols], lo.at[z, 2]))
            w, m, v = ((wg_h, mg_h, vg_h), (wu_h, mu_h, vu_h))[which]
            return (load(w.at[layer, first, cols], cw.at[z], lp.at[z, 0]), load(m.at[layer, :, cols], cm.at[z], lp.at[z, 1]),
                    load(v.at[layer, :, cols], cv.at[z], lp.at[z, 2]))
        if out:
            return (load(fw.at[z], od_h.at[layer, mx, my, mine, :], lo.at[z, 0]), load(fm.at[z], omd_h.at[layer, mine, :], lo.at[z, 1]),
                    load(fv.at[z], ovd_h.at[layer, mine, :], lo.at[z, 2]))
        return (load(wd_h.at[layer, rows, :], ew.at[z], lp.at[z, 0]), load(md_h.at[layer, mine, :], em.at[z], lp.at[z, 1]),
                load(vd_h.at[layer, mine, :], ev.at[z], lp.at[z, 2]))

    def on_matrix(u, do):
        k = lax.rem(u, per_layer)
        down = k >= 2 * BLOCKS
        for which, test in enumerate((~down & (lax.rem(k, 2) == 0), ~down & (lax.rem(k, 2) == 1), down)):
            pl.when(test)(functools.partial(do, which))

    def out_at(u, i, which):
        layer, j = place(u)
        if which < 2:
            cols = pl.ds(pl.multiple_of(j * f, LANES), f)
            return lambda x, y: (og_h, ou_h)[which].at[layer, x, y, pl.ds(i * sub_g, sub_g), cols]
        rows = pl.ds(pl.multiple_of(j * sub_d, 8), sub_d)
        wide = d // KINDS
        return lambda x, y: od_h.at[layer, x, y, rows, pl.ds(i * wide, wide)]

    def s4_copies(u, i, which):
        _, _, ahead, behind, _, _, _ = steps(i)
        z = lax.rem(u, 2)
        wide = d // KINDS
        dst = out_at(u, i, which)(mx, my)
        src = nw.at[z, pl.ds(i * sub_g, sub_g), :] if which < 2 else fw.at[z, :, pl.ds(i * wide, wide)]
        return (rcopy(src, dst, u, i, 6, ahead), rcopy(src, dst, u, i, 7, behind))

    def s5_copy(u, i, which):
        _, _, ahead, _, pf, ps, s = steps(i)
        at = out_at(u, i, which)
        src = at(pf, wrap(ps - s)) if i < 2 else at(wrap(ps - s), pf)
        return rcopy(src, src, u, i, 8, ahead)

    every = pl.ds(0, SIDE)

    def s6_copies(u, i, which):
        ahead, behind, _, _, pf, _, _ = steps(i)
        at = out_at(u, i, which)
        src = at(pf, every) if i < 2 else at(every, pf)
        return (rcopy(src, src, u, i, 9, ahead), rcopy(src, src, u, i, 10, behind))

    def s7_copy(u, i, which):
        ahead, _, _, _, pf, _, s = steps(i)
        at = out_at(u, i, which)
        p = wrap(pf - s)
        src = at(p, every) if i < 2 else at(every, p)
        return rcopy(src, src, u, i, 11, ahead)

    def stage0(u):
        def do(which):
            for i in range(KINDS):
                start(*s0_copies(u, i, which))
        on_own(u, do)

    def stage1(u):
        n_ = lax.rem(u, SLOTS)

        def do(which):
            for i in range(KINDS):
                _, _, _, _, pf, _, s = steps(i)
                wait(s0_copies(u, i, which)[0])
                mine = own(u, i, wrap(pf + s), which)
                r1[n_, i] = (r1[n_, i].astype(F32) + mine[...].astype(F32)).astype(BF)
                start(s1_copy(u, i))
        on_own(u, do)

    def stage2(u):
        n_ = lax.rem(u, SLOTS)

        def do(which):
            for i in range(KINDS):
                _, _, _, _, pf, ps, s = steps(i)
                wait(s0_copies(u, i, which)[1], s1_copy(u, i))
                mine = own(u, i, pf, which)
                for k in (2, -s, s, 0):
                    p = wrap(ps + k)
                    total = r2[n_, i, p].astype(F32) + r3[n_, i, p].astype(F32) + mine[p].astype(F32)
                    if k in (2, -s):
                        r3[n_, i, p] = total.astype(BF)
                    else:
                        t3[n_, i, 0 if k else 1] = total
                start(*s2_copies(u, i))
        on_own(u, do)

    def stage3(u):
        n_ = lax.rem(u, SLOTS)
        on_matrix(u, lambda which: start(*state_copies(u, which, False)))
        for i in range(KINDS):
            wait(s2_copies(u, i)[0])
            q1[n_, i] = (q1[n_, i].astype(F32) + t3[n_, i, 0]).astype(BF)
            start(s3_copy(u, i))

    def stage4(u):
        n_, z = lax.rem(u, SLOTS), lax.rem(u, 2)

        def update(g, w, m, v):
            g = g.astype(BF).astype(F32)
            m = 0.9 * m + 0.1 * g
            v = 0.95 * v + 0.05 * g * g
            w = w.astype(F32)
            return (w - 0.02 * (m * lax.rsqrt(v + 1e-8) + 0.1 * w)).astype(BF), m, v

        for i in range(KINDS):
            wait(s2_copies(u, i)[1], s3_copy(u, i))

        def do(which):
            wait(*state_copies(u, which, False))
            wide, sub = d // KINDS, sub_g if which < 2 else sub_d
            for i in range(KINDS):
                for c in range(r1.shape[3] // sub):
                    part = pl.ds(c * sub, sub)
                    g = q2[n_, i, part, :].astype(F32) + q3[n_, i, part, :].astype(F32) + t3[n_, i, 1, part, :]
                    if which < 2:
                        at = (z, pl.ds(i * sub, sub), pl.ds(c * LANES, LANES))
                        nw[at], nm[at], nv[at] = update(g, cw[at], cm[at], cv[at])
                    else:
                        at = (z, slice(None), pl.ds(i * wide + c * LANES, LANES))
                        fw[at], fm[at], fv[at] = update(g, ew[at], em[at], ev[at])
                start(*s4_copies(u, i, which))
            start(*state_copies(u, which, True))
        on_matrix(u, do)

    def stage5(u):
        def do(which):
            wait(*state_copies(u, which, True))
            for i in range(KINDS):
                wait(*s4_copies(u, i, which))
                start(s5_copy(u, i, which))
        on_matrix(u, do)

    def stage6(u):
        def do(which):
            for i in range(KINDS):
                wait(s5_copy(u, i, which))
                start(*s6_copies(u, i, which))
        on_matrix(u, do)

    def stage7(u):
        def do(which):
            for i in range(KINDS):
                wait(*s6_copies(u, i, which))
                start(s7_copy(u, i, which))
        on_matrix(u, do)

    def stage8(u):
        def do(which):
            for i in range(KINDS):
                wait(s7_copy(u, i, which))
        on_matrix(u, do)

    stages = (stage0, stage1, stage2, stage3, stage4, stage5, stage6, stage7, stage8)
    parts, first = 2, 4

    last = layers - 1
    in_a = n // rows_d

    def keep():
        def some(o, _):
            x, y = o // SIDE, lax.rem(o, SIDE)
            to = pl.ds(pl.multiple_of(o * rows_g, 8), rows_g)
            for k, (w, wide) in enumerate(((og_h, wgu), (ou_h, both))):
                half = pl.ds(pl.multiple_of(k * d + o * rows_g, 8), rows_g)
                for c in range(2):
                    at = wide.at[c, to] if k == 0 else wide.at[pl.ds(pl.multiple_of(c * d + o * rows_g, 8), rows_g)]
                    start(load(w.at[last, x, y, :, pl.ds(c * 2 * f, 2 * f)], at, lf.at[2 * k + c]))
                start(load(w.at[last, x, y, :, pl.ds(4 * f, f)], hid.at[half], lf.at[4 + k]))
                start(load(w.at[0, x, y, :, pl.ds(0, d)], dy.at[half], lf.at[6 + k]))

            @pl.when(o < in_a)
            def _():
                start(load(od_h.at[last, x, y], a.at[pl.ds(pl.multiple_of(o * rows_d, 8), rows_d)], lf.at[8]))

            @pl.when(o >= in_a)
            def _():
                start(load(od_h.at[last, x, y], h.at[pl.ds(pl.multiple_of((o - in_a) * rows_d, 8), rows_d)], lf.at[9]))
            return 0

        lax.fori_loop(0, SIDE * SIDE, some, 0)

    def kept():
        half = pl.ds(0, d)
        for c in range(2):
            wait(load(both_h.at[0, half], wgu.at[c], lf.at[c]), load(both_h.at[0, half], both.at[pl.ds(c * d, d)], lf.at[2 + c]))
        for k in range(2):
            wait(load(both_h.at[0, half, pl.ds(0, f)], hid.at[pl.ds(k * d, d)], lf.at[4 + k]),
                 load(dy_h.at[half], dy.at[pl.ds(k * d, d)], lf.at[6 + k]))
        for k, (blocks, to) in enumerate(((in_a, a), (SIDE * SIDE - in_a, h))):
            rows = pl.ds(0, blocks * rows_d)
            wait(load(dy_h.at[rows], to.at[rows], lf.at[8 + k]))

    keep_at = max(first + parts * (per_layer + 3) + WHEN[-1] + 1, parts * (per_layer + 2 * BLOCKS))
    assert d <= 2 * f

    def tick(t, _):
        for when, stage in zip(WHEN, stages, strict=True):
            since = t - first - when + parts * WHEN[-1]
            u = since // parts - WHEN[-1]
            pl.when((u >= 0) & (u < units) & (lax.rem(since, parts) == 0))(functools.partial(stage, u))
        pl.when(t == keep_at)(keep)

        layer = layers - 1 - t // (parts * per_layer)
        k = lax.rem(t, parts * per_layer)
        b, piece, c = k // 4, lax.rem(k, 4), k - 4 * BLOCKS
        busy, blocks, u = t < parts * units, k < 4 * BLOCKS, (layers - 1 - layer) * per_layer + 2 * b
        pl.when(busy & blocks & (piece < 2))(lambda: hidden_units(layer, b, piece))
        pl.when(busy & blocks & (piece == 2))(lambda: gradient_columns(u, 0, SIDE - 1))

        @pl.when(busy & blocks & (piece == 3))
        def _():
            gradient_columns(u, SIDE - 1, SIDE)
            gradient_rows(layer, b)

        pl.when(busy & ~blocks & (layer > 0))(lambda: states_back(c // 2, lax.rem(c, 2)))
        return 0

    first_units(0)
    start(load_dy)
    lax.fori_loop(1, BLOCKS - 1, lambda b, _: (first_units(b), 0)[1], 0)
    first_units(BLOCKS - 1)
    pl.semaphore_wait(barrier, 4)
    lax.fori_loop(0, first + parts * (units - 1) + WHEN[-1] + 1, tick, 0)
    kept()


def results_kernel(*refs, hidden, count):
    (og, ou, od), moments, kept = refs[:3], refs[3:9], refs[9:15]
    (rg, ru, rd), moved = refs[15:18], refs[18:24]
    bg, bu, bd, bufs, sems = refs[24], refs[25], refs[26], refs[27:33], refs[33]
    a, h, dy, wgu, hid, both = kept
    n, d = a.shape
    f, last = hid.shape[1], rg.shape[0] - 1
    copies = []

    def copy(src, dst):
        copies.append(pltpu.make_async_copy(src, dst, sems.at[len(copies)]))
        return copies[-1]

    through = []
    step = d // 4
    for w, buf, out in ((og, bg, rg), (ou, bu, ru)):
        for r in range(0, d, step):
            at = (pl.ds(r, step), pl.ds(d, hidden - d))
            through.append((copy(w.at[0, *at], buf.at[pl.ds(r, step)]), copy(buf.at[pl.ds(r, step)], out.at[0, *at])))
    step = hidden // 4
    for r in range(0, hidden, step):
        at = pl.ds(r, step)
        through.append((copy(od.at[0, at], bd.at[at]), copy(bd.at[at], rd.at[0, at])))
    for src, buf, out in zip(moments, bufs, moved, strict=True):
        for layer in range(last + 1):
            through.append((copy(src.at[layer], buf.at[layer]), copy(buf.at[layer], out.at[layer])))
    block = hidden // (SIDE * SIDE)
    rows = n // block * block
    straight = [copy(a.at[pl.ds(0, rows)], rd.at[last, pl.ds(0, rows)]), copy(h.at[pl.ds(0, hidden - rows)], rd.at[last, pl.ds(rows, hidden - rows)])]
    for k, out in enumerate((rg, ru)):
        for c in range(2):
            src = both.at[pl.ds(c * d, d)] if k else wgu.at[c]
            straight.append(copy(src, out.at[last, :, pl.ds(c * 2 * f, 2 * f)]))
        straight.append(copy(hid.at[pl.ds(k * d, d)], out.at[last, :, pl.ds(4 * f, f)]))
        straight.append(copy(dy.at[pl.ds(k * d, d)], out.at[0, :, pl.ds(0, d)]))
    assert len(copies) == count
    for i, _ in through:
        i.start()
    for c in straight:
        c.start()
    for i, o in through:
        i.wait()
        o.start()
    for c in (*straight, *(o for _, o in through)):
        c.wait()


def results(arrays, kept):
    (layers, d, hidden), moments = arrays[0].shape, arrays[3:]
    count = 2 * (4 + 4 + 4 + len(moments) * layers) + 10
    vmem = [pltpu.VMEM(s, t) for s, t in (((d, hidden - d), BF), ((d, hidden - d), BF), ((hidden, d), BF), *((m.shape, F32) for m in moments))]
    return pl.pallas_call(
        functools.partial(results_kernel, hidden=hidden, count=count),
        out_shape=[jax.ShapeDtypeStruct(a.shape, a.dtype) for a in arrays],
        in_specs=[pl.BlockSpec(memory_space=pltpu.HBM)] * len(arrays) + [pl.BlockSpec(memory_space=pltpu.VMEM)] * len(kept),
        out_specs=[pl.BlockSpec(memory_space=pltpu.HBM)] * len(arrays),
        scratch_shapes=vmem + [pltpu.SemaphoreType.DMA((count,))],
        compiler_params=pltpu.CompilerParams(vmem_limit_bytes=VLIM),
        name="results",
    )(*(pltpu.with_memory_space_constraint(a, pltpu.HBM) for a in arrays), *(pltpu.with_memory_space_constraint(a, pltpu.VMEM) for a in kept))


def train_step(layers, x, dy, ws, ms, vs):
    n, d = dy.shape
    f = ws[0].shape[2] // BLOCKS
    owners = SIDE * SIDE
    rows_g, rows_d = d // owners, f * BLOCKS // owners
    units = layers * 3 * BLOCKS
    ring = 4
    flat = rows_g * f // KINDS // LANES
    blocks = (SLOTS, KINDS, SIDE, flat, LANES)
    block = (SLOTS, KINDS, flat, LANES)
    gate, down = (2, rows_g, f), (2, rows_d // BLOCKS, d)
    vmem, dma = pltpu.VMEM, pltpu.SemaphoreType.DMA
    sd = jax.ShapeDtypeStruct
    outs = pl.pallas_call(
        functools.partial(step_kernel, layers=layers, units=units, ring=ring),
        out_shape=[sd((layers, SIDE, SIDE, rows_g, f * BLOCKS), BF)] * 2
        + [sd((layers, SIDE, SIDE, rows_d, d), BF)]
        + [sd(m.shape, F32) for m in ms] + [sd(v.shape, F32) for v in vs]
        + [sd((BLOCKS, n, 2 * f), BF)]
        + [vmem((n, d), BF)] * 3 + [vmem((2, d, 2 * f), BF), vmem((n, f), BF), vmem((n, 2 * f), BF)],
        in_specs=[ANY] * 11,
        out_specs=[ANY] * 10 + [pl.BlockSpec(memory_space=pltpu.VMEM)] * 6,
        scratch_shapes=[
            vmem((2, f, d), BF), vmem((n, d), F32),
            vmem((ring, KINDS, SIDE, SIDE, flat, LANES), BF), vmem((BLOCKS + 1, KINDS, SIDE, SIDE, flat, LANES), BF),
            vmem(blocks, BF), vmem(blocks, BF), vmem(blocks, BF), vmem((SLOTS, KINDS, 2, flat, LANES), F32),
            vmem(block, BF), vmem(block, BF), vmem(block, BF),
            vmem(gate, BF), vmem(gate, F32), vmem(gate, F32), vmem(gate, BF), vmem(gate, F32), vmem(gate, F32),
            vmem(down, BF), vmem(down, F32), vmem(down, F32), vmem(down, BF), vmem(down, F32), vmem(down, F32),
            dma((SLOTS, KINDS, 12)), dma((SLOTS, KINDS, 12)),
            dma((2, 3)), dma((n // 256,)), dma((2,)), dma, dma((2, 3)), dma((2, 3)), dma((10,)),
        ],
        compiler_params=pltpu.CompilerParams(collective_id=0, has_side_effects=True, vmem_limit_bytes=VLIM),
        name="train_step",
    )(x, dy, *ws, *ms, *vs)
    return outs[:9], outs[10:]


def solution(mesh):
    assert mesh.shape["dp"] == SIDE * SIDE

    def body(x, dy, *arrays):
        ws, ms, vs = (arrays[i : i + 3] for i in (0, 3, 6))
        x, dy = x[0], dy[0]
        layers = ws[0].shape[0]
        outs, kept = train_step(layers, x, dy, ws, ms, vs)
        return tuple(results([o.reshape(w.shape) for o, w in zip(outs[:3], ws, strict=True)] + list(outs[3:]), kept))

    whole, rows = P(None, None, None), P(None, "dp", None)
    return jax.shard_map(
        body,
        mesh=mesh,
        in_specs=(P(("rep", "dp")),) * 2 + (whole,) * 3 + (rows,) * 6,
        out_specs=(P("rep"),) * 3 + (P("rep", "dp"),) * 6,
        check_vma=False,
    )
```
